16 devices in a mesh: data: 4 (over z, y), model: 4 (over x, core).
Axes of the slice: x: 2, y: 2, z: 2, core: 2. Of those that a mesh axis runs over, the one named last changes fastest.
Arguments:
- hidden_in: bfloat16 [512, 3584], P('data'), parts along dimension 0
- positions: int32 [512], P('data'), parts along dimension 0
- norm_attn: bfloat16 [3, 3584], replicated
- norm_mlp: bfloat16 [3, 3584], replicated
- w_query: bfloat16 [3, 3584, 3584], P(None, None, 'model')
- w_key: bfloat16 [3, 3584, 512], P(None, None, 'model')
- w_value: bfloat16 [3, 3584, 512], P(None, None, 'model')
- w_out: bfloat16 [3, 3584, 3584], P(None, 'model')
- w_gate: bfloat16 [3, 3584, 18944], P(None, None, 'model')
- w_up: bfloat16 [3, 3584, 18944], P(None, None, 'model')
- w_down: bfloat16 [3, 18944, 3584], P(None, 'model')
- key_cache: bfloat16 [3, 512, 32, 4, 128], P(None, 'data', None, 'model'), parts along dimension 1
- value_cache: bfloat16 [3, 512, 32, 4, 128], P(None, 'data', None, 'model'), parts along dimension 1
Outputs:
- output 1: bfloat16 [512, 3584], P('data'), parts along dimension 0
- output 2: bfloat16 [3, 512, 32, 4, 128], P(None, 'data', None, 'model'), parts along dimension 1
- output 3: bfloat16 [3, 512, 32, 4, 128], P(None, 'data', None, 'model'), parts along dimension 1
There are 4 independent parts. The reference program is written for one: setup_inputs(seed, part) draws one part's arguments, and reference() takes and returns one part's arrays. A program takes and returns all parts, laid end to end along the dimension named above; an argument that names none is the same for every part.
All inputs are finite; a program needn't handle non-finite values.
Results may differ from the reference program's by a relative error of at most 0.02.
Values are sent between devices in bfloat16 or wider.
A program may use at most 1.5 GiB of HBM per device.

```python
import math
import jax
import jax.numpy as jnp
from jax import lax

LAYERS = 3
BATCH = 128
CACHE_LEN = 32
MODEL_DIM = 3584
HEADS = 28
KV_HEADS = 4
HEAD_DIM = 128
FF_DIM = 18944
NORM_EPS = 1e-6
ROPE_BASE = 10000.0


def setup_inputs(seed: int = 0, part: int = 0) -> dict:
    root = jax.random.key(seed)
    shared = jax.random.split(root, 9)
    local = jax.random.split(jax.random.fold_in(root, part), 6)
    q_width = HEADS * HEAD_DIM
    kv_width = KV_HEADS * HEAD_DIM
    key_scale = math.sqrt(math.log(CACHE_LEN / 4.0))
    hidden_in = jax.random.normal(local[0], (BATCH, MODEL_DIM), jnp.float32).astype(jnp.bfloat16)
    positions = jax.random.randint(local[1], (BATCH,), 0, CACHE_LEN, dtype=jnp.int32)
    top_row = jax.random.randint(local[2], (), 0, BATCH, dtype=jnp.int32)
    positions = jnp.where(jnp.arange(BATCH) == top_row, CACHE_LEN - 1, positions).astype(jnp.int32)
    norm_attn = jax.random.uniform(shared[0], (LAYERS, MODEL_DIM), jnp.float32, 0.5, 1.5).astype(jnp.bfloat16)
    norm_mlp = jax.random.uniform(shared[1], (LAYERS, MODEL_DIM), jnp.float32, 0.5, 1.5).astype(jnp.bfloat16)
    w_query = (jax.random.normal(shared[2], (LAYERS, MODEL_DIM, q_width), jnp.float32) * MODEL_DIM ** -0.5).astype(jnp.bfloat16)
    w_key = (jax.random.normal(shared[3], (LAYERS, MODEL_DIM, kv_width), jnp.float32) * (key_scale * MODEL_DIM ** -0.5)).astype(jnp.bfloat16)
    w_value = (jax.random.normal(shared[4], (LAYERS, MODEL_DIM, kv_width), jnp.float32) * MODEL_DIM ** -0.5).astype(jnp.bfloat16)
    w_out = (jax.random.normal(shared[5], (LAYERS, q_width, MODEL_DIM), jnp.float32) * q_width ** -0.5).astype(jnp.bfloat16)
    w_gate = (jax.random.normal(shared[6], (LAYERS, MODEL_DIM, FF_DIM), jnp.float32) * MODEL_DIM ** -0.5).astype(jnp.bfloat16)
    w_up = (jax.random.normal(shared[7], (LAYERS, MODEL_DIM, FF_DIM), jnp.float32) * MODEL_DIM ** -0.5).astype(jnp.bfloat16)
    w_down = (jax.random.normal(shared[8], (LAYERS, FF_DIM, MODEL_DIM), jnp.float32) * FF_DIM ** -0.5).astype(jnp.bfloat16)
    cache_shape = (LAYERS, BATCH, CACHE_LEN, KV_HEADS, HEAD_DIM)
    key_cache = (jax.random.normal(local[3], cache_shape, jnp.float32) * key_scale).astype(jnp.bfloat16)
    value_mean = jax.random.normal(local[4], (LAYERS, BATCH, 1, KV_HEADS, HEAD_DIM), jnp.float32)
    value_cache = (value_mean + jax.random.normal(local[5], cache_shape, jnp.float32)).astype(jnp.bfloat16)
    return {"hidden_in": hidden_in, "positions": positions, "norm_attn": norm_attn, "norm_mlp": norm_mlp, "w_query": w_query, "w_key": w_key, "w_value": w_value, "w_out": w_out, "w_gate": w_gate, "w_up": w_up, "w_down": w_down, "key_cache": key_cache, "value_cache": value_cache}


def rms_norm(vals, gain):
    vals_f = vals.astype(jnp.float32)
    inv_rms = lax.rsqrt(jnp.mean(vals_f * vals_f, axis=-1, keepdims=True) + NORM_EPS)
    return (vals_f * inv_rms * gain.astype(jnp.float32)).astype(jnp.bfloat16)


def rope_tables(positions):
    half = HEAD_DIM // 2
    inv_freq = ROPE_BASE ** (-jnp.arange(half, dtype=jnp.float32) / half)
    angles = positions.astype(jnp.float32)[:, None] * inv_freq[None, :]
    return jnp.cos(angles), jnp.sin(angles)


def apply_rope(vals, cos_tab, sin_tab):
    half = HEAD_DIM // 2
    vals_f = vals.astype(jnp.float32)
    first = vals_f[..., :half]
    second = vals_f[..., half:]
    cos_b = cos_tab[:, None, :]
    sin_b = sin_tab[:, None, :]
    return jnp.concatenate([first * cos_b - second * sin_b, second * cos_b + first * sin_b], axis=-1).astype(jnp.bfloat16)


def reference(hidden_in, positions, norm_attn, norm_mlp, w_query, w_key, w_value, w_out, w_gate, w_up, w_down, key_cache, value_cache):
    cos_tab, sin_tab = rope_tables(positions)
    slots = jnp.arange(CACHE_LEN)
    write_row = (slots[None, :] == positions[:, None])[:, :, None, None]
    visible = (slots[None, :] <= positions[:, None])[:, None, None, :]
    group = HEADS // KV_HEADS
    scale = HEAD_DIM ** -0.5

    def layer_step(residual, layer_args):
        g_attn, g_mlp, q_proj, k_proj, v_proj, o_proj, gate_proj, up_proj, down_proj, k_cache, v_cache = layer_args
        hidden = rms_norm(residual, g_attn)
        query = jnp.dot(hidden, q_proj, preferred_element_type=jnp.float32).astype(jnp.bfloat16).reshape(BATCH, HEADS, HEAD_DIM)
        key_new = jnp.dot(hidden, k_proj, preferred_element_type=jnp.float32).astype(jnp.bfloat16).reshape(BATCH, KV_HEADS, HEAD_DIM)
        value_new = jnp.dot(hidden, v_proj, preferred_element_type=jnp.float32).astype(jnp.bfloat16).reshape(BATCH, KV_HEADS, HEAD_DIM)
        query = apply_rope(query, cos_tab, sin_tab)
        key_new = apply_rope(key_new, cos_tab, sin_tab)
        k_cache = jnp.where(write_row, key_new[:, None], k_cache)
        v_cache = jnp.where(write_row, value_new[:, None], v_cache)
        query_g = query.reshape(BATCH, KV_HEADS, group, HEAD_DIM)
        scores = jnp.einsum("bkgd,bskd->bkgs", query_g.astype(jnp.float32), k_cache.astype(jnp.float32)) * scale
        scores = jnp.where(visible, scores, -1e30)
        attn_prob = jax.nn.softmax(scores, axis=-1).astype(jnp.bfloat16)
        attn_val = jnp.einsum("bkgs,bskd->bkgd", attn_prob.astype(jnp.float32), v_cache.astype(jnp.float32)).astype(jnp.bfloat16).reshape(BATCH, HEADS * HEAD_DIM)
        residual = (residual.astype(jnp.float32) + jnp.dot(attn_val, o_proj, preferred_element_type=jnp.float32)).astype(jnp.bfloat16)
        hidden = rms_norm(residual, g_mlp)
        gate_pre = jnp.dot(hidden, gate_proj, preferred_element_type=jnp.float32)
        up_val = jnp.dot(hidden, up_proj, preferred_element_type=jnp.float32)
        act_val = (jax.nn.silu(gate_pre) * up_val).astype(jnp.bfloat16)
        residual = (residual.astype(jnp.float32) + jnp.dot(act_val, down_proj, preferred_element_type=jnp.float32)).astype(jnp.bfloat16)
        return residual, (k_cache, v_cache)

    final, caches = lax.scan(layer_step, hidden_in, (norm_attn, norm_mlp, w_query, w_key, w_value, w_out, w_gate, w_up, w_down, key_cache, value_cache))
    return final, caches[0], caches[1]
```

```python
import functools

import jax
import jax.numpy as jnp
import numpy as np
from jax import lax
from jax.experimental import pallas as pl
from jax.experimental.pallas import tpu as pltpu
from jax.sharding import PartitionSpec as P

NORM_EPS = 1e-6
ROPE_BASE = 10000.0
MESH = pl.DeviceIdType.MESH
F32 = jnp.float32
BF16 = jnp.bfloat16

LAYERS = 3
ROWS = 128
DIM = 3584
HD = 128
QH = 7
CACHE = 32
FF = 4736
BLKS = DIM // 128
CH = DIM // 256
PAIRS = DIM // 512
QKV = (QH + 2) * HD
PER_LAYER = 4 + 4 + 4 * PAIRS + CH
TOTAL = LAYERS * PER_LAYER
SLOTS = 17
DOWN = 2.0 ** -32
UP = 2.0 ** 32
GROUP = 8
UNROLL = 8


def kernel(x_hbm, pos_ref, na_ref, nm_ref, freq_ref, wq, wk, wv, wo, wg, wu, wd, kc_hbm, vc_hbm,
           out_hbm, kn_out, vn_out,
           ring, ring_sem, x, x_sem, gn, posb, cos_t, sin_t, vis, ss, qkv, qs, kn, vn, at, ab, acc_g, acc_u, act,
           kbuf, vbuf, kv_sem, own, a_send, a_recv, b_send, b_recv, a_ss, a_rs, b_ss, b_rs, c_ss, c_rs):
    me = lax.axis_index("model")
    core = lax.rem(me, 2)
    partner = me + 1 - 2 * core
    peer = lax.rem(me + 2, 4)

    def slot_of(n):
        return lax.rem(n, SLOTS)

    def issue(n):
        layer = n // PER_LAYER
        r = n - layer * PER_LAYER
        s = slot_of(n)
        live = n < TOTAL

        def copy(src, dst):
            pltpu.make_async_copy(src, dst, ring_sem.at[s]).start()

        def qkv_part(r, parts):
            for t in range(parts):
                rows = pl.ds(pl.multiple_of((r * 4 + t) * 256, 256), 256)
                base = t * QKV
                copy(wq.at[layer, rows, :], ring.at[s, :, base:base + QH * HD])
                copy(wk.at[layer, rows, :], ring.at[s, :, base + QH * HD:base + (QH + 1) * HD])
                copy(wv.at[layer, rows, :], ring.at[s, :, base + (QH + 1) * HD:base + QKV])

        @pl.when(live & (r < 3))
        def _():
            qkv_part(r, 4)

        @pl.when(live & (r == 3))
        def _():
            qkv_part(3, 2)

        @pl.when(live & (r >= 4) & (r < 7))
        def _():
            copy(wo.at[layer, pl.ds(pl.multiple_of((r - 4) * 256, 256), 256), :], ring.at[s, :, :DIM])

        @pl.when(live & (r == 7))
        def _():
            copy(wo.at[layer, 768:896, :], ring.at[s, :128, :DIM])

        gu = r - 8
        row0 = 512 * (gu // 4) + 256 * lax.rem(gu, 2)

        @pl.when(live & (r >= 8) & (r < 36) & (lax.rem(gu, 4) < 2))
        def _():
            copy(wg.at[layer, pl.ds(pl.multiple_of(row0, 256), 256), :], ring.at[s])

        @pl.when(live & (r >= 8) & (r < 36) & (lax.rem(gu, 4) >= 2))
        def _():
            copy(wu.at[layer, pl.ds(pl.multiple_of(row0, 256), 256), :], ring.at[s])

        @pl.when(live & (r >= 36))
        def _():
            cols = pl.ds(pl.multiple_of((r - 36) * 256, 256), 256)
            for b in range(18):
                copy(wd.at[layer, b * 256:b * 256 + 256, cols], ring.at[s, :, b * 256:b * 256 + 256])
            c0 = pl.ds(pl.multiple_of((r - 36) * 256, 128), 128)
            c1 = pl.ds(pl.multiple_of((r - 36) * 256 + 128, 128), 128)
            copy(wd.at[layer, 4608:4736, c0], ring.at[s, :128, 4608:4736])
            copy(wd.at[layer, 4608:4736, c1], ring.at[s, 128:, 4608:4736])

    def wait_slot(n, rows, cols):
        s = slot_of(n)
        pltpu.make_async_copy(wg.at[0, :rows, :cols], ring.at[s, :rows, :cols], ring_sem.at[s]).wait()

    def kv_copies(layer):
        b = lax.rem(layer, 2)
        return (pltpu.make_async_copy(kc_hbm.at[layer], kbuf.at[b], kv_sem.at[0, b]),
                pltpu.make_async_copy(vc_hbm.at[layer], vbuf.at[b], kv_sem.at[1, b]))

    barrier = pltpu.get_barrier_semaphore()
    for other in (partner, peer):
        pl.semaphore_signal(barrier, inc=1, device_id={"model": other}, device_id_type=MESH)

    def load_x(b, carry):
        pltpu.make_async_copy(x_hbm.at[:, pl.ds(pl.multiple_of(b * 128, 128), 128)], x.at[b], x_sem).start()
        return carry

    lax.fori_loop(0, BLKS, load_x, 0)

    def prologue(n, carry):
        issue(n)
        return carry

    lax.fori_loop(0, 4, prologue, 0)
    for cp in kv_copies(0):
        cp.start()
    lax.fori_loop(4, SLOTS, prologue, 0)

    for layer in range(LAYERS):
        for which, ref in enumerate((na_ref, nm_ref)):
            row = ref[layer:layer + 1, :].astype(F32) * DOWN
            gn[2 * layer + which] = jnp.broadcast_to(row, (8, DIM))
    pos_row = jnp.broadcast_to(pos_ref[...].astype(F32), (ROWS, ROWS))
    ri = lax.broadcasted_iota(jnp.int32, (ROWS, ROWS), 0)
    ci = lax.broadcasted_iota(jnp.int32, (ROWS, ROWS), 1)
    pos_col = jnp.sum(jnp.where(ri == ci, pos_row, 0.0), axis=1, keepdims=True)
    pos_b = jnp.broadcast_to(pos_col, (ROWS, HD))
    posb[...] = pos_b
    angle = pos_b * freq_ref[...]
    cos_t[...] = jnp.cos(angle)
    sin_v = jnp.sin(angle)
    sin_t[...] = jnp.where(ci < HD // 2, -sin_v, sin_v)
    r2 = lax.broadcasted_iota(jnp.int32, (ROWS, GROUP * CACHE), 0)
    c2 = lax.broadcasted_iota(jnp.int32, (ROWS, GROUP * CACHE), 1)
    mine = (c2 // CACHE) == lax.rem(r2, GROUP)
    seen = lax.rem(c2, CACHE).astype(F32) <= jnp.broadcast_to(pos_col, (ROWS, GROUP * CACHE))
    vis[...] = jnp.where(mine & seen, 1.0, 0.0)

    pltpu.make_async_copy(x, x, x_sem).wait()
    pl.semaphore_wait(barrier, 2)

    def a_copy(j):
        return pltpu.make_async_remote_copy(a_send.at[j], a_recv.at[j], a_ss.at[j], a_rs.at[j],
                                            device_id={"model": partner}, device_id_type=MESH)

    def b_copy(p, j):
        return pltpu.make_async_remote_copy(b_send.at[j], b_recv.at[p, j], b_ss.at[j], b_rs.at[p, j],
                                            device_id={"model": peer}, device_id_type=MESH)

    def c_copy(j, half):
        blk = 2 * j + half
        return pltpu.make_async_remote_copy(x.at[blk], x.at[blk], c_ss.at[j], c_rs.at[j],
                                            device_id={"model": partner}, device_id_type=MESH)

    def stage_a(j, part):
        lo, hi = part[:, :128], part[:, 128:]
        first = core == 0
        own[j] = jnp.where(first, lo, hi)
        a_send[j] = jnp.where(first, hi, lo).astype(BF16)
        a_copy(j).start()

    def stage_b(p, j):
        a_copy(j).wait_recv()
        b_send[j] = (own[j] + a_recv[j].astype(F32)).astype(BF16)
        b_copy(p, j).start()

    def stage_c(p, j):
        b_copy(p, j).wait_recv()
        total = b_send[j].astype(F32) + b_recv[p, j].astype(F32)
        blk = 2 * j + core
        x[blk] = (x[blk].astype(F32) + total).astype(BF16)
        c_copy(j, core).start()
        a_copy(j).wait_send()
        b_copy(p, j).wait_send()

    def stage_d(j):
        c_copy(j, 1 - core).wait_recv()
        c_copy(j, core).wait_send()

    def stage_c2(p, i):
        stage_c(p, 2 * i)
        stage_c(p, 2 * i + 1)

    def stage_d2(i):
        stage_d(2 * i)
        stage_d(2 * i + 1)

    def take(row, i):
        outs = []
        sq = ss[...]
        for b in range(4):
            blk = x[4 * i + b].astype(F32)
            sq = sq + blk * blk
            gain = gn[row, 0:1, pl.ds(pl.multiple_of(i * 512 + b * 128, 128), 128)]
            outs.append((blk * gain).astype(BF16))
        ss[...] = sq
        return (jnp.concatenate(outs[:2], axis=1), jnp.concatenate(outs[2:], axis=1))

    def row_scale():
        mean = jnp.sum(ss[...], axis=1, keepdims=True) * (1.0 / DIM)
        return lax.rsqrt(mean + NORM_EPS) * UP

    def dot(a, b):
        return jnp.dot(a, b, preferred_element_type=F32)

    def tiles(width, step):
        return [(n, min(step, width - n)) for n in range(0, width, step)]

    def layer_body(layer, carry):
        base = layer * PER_LAYER
        ss[...] = jnp.zeros_like(ss)
        qkv[...] = jnp.zeros_like(qkv)

        @pl.when(layer > 0)
        def _():
            stage_c2(1, 0)

        def qkv_step(i, carry):
            @pl.when((layer > 0) & (i + 1 < PAIRS))
            def _():
                stage_c2(1, i + 1)

            @pl.when(layer > 0)
            def _():
                stage_d2(i)

            n = base + i // 2
            half = lax.rem(i, 2)

            @pl.when((half == 0) & (i < 6))
            def _():
                wait_slot(n, 256, 4 * QKV)

            @pl.when(i == 6)
            def _():
                wait_slot(n, 256, 2 * QKV)

            h0, h1 = take(2 * layer, i)
            s = slot_of(n)
            for c0, w in tiles(QKV, 512):
                o0 = pl.ds(pl.multiple_of(half * 2 * QKV + c0, 128), w)
                o1 = pl.ds(pl.multiple_of(half * 2 * QKV + QKV + c0, 128), w)
                qkv[:, c0:c0 + w] += dot(h0, ring[s, :, o0]) + dot(h1, ring[s, :, o1])

            @pl.when((half == 1) | (i == 6))
            def _():
                issue(n + SLOTS)

            return carry

        lax.fori_loop(0, PAIRS, qkv_step, 0)

        scale = row_scale()
        cos_v, sin_v = cos_t[...], sin_t[...]

        def head(idx):
            return (qkv[:, idx * HD:(idx + 1) * HD] * scale).astype(BF16)

        def rotate(v):
            v = v.astype(F32)
            return (v * cos_v + pltpu.roll(v, HD // 2, axis=1) * sin_v).astype(BF16)

        for h in range(QH):
            qs[h] = rotate(head(h)).astype(F32)
        k_new = rotate(head(QH))
        v_new = head(QH + 1)
        kn[...] = k_new.astype(F32)
        vn[...] = v_new.astype(F32)
        kn_out[layer] = k_new
        vn_out[layer] = v_new
        for cp in kv_copies(layer):
            cp.wait()
        buf = lax.rem(layer, 2)
        srow = lax.rem(lax.broadcasted_iota(jnp.int32, (GROUP * CACHE, HD), 0), CACHE).astype(F32)

        def spread(v):
            return jnp.broadcast_to(v[:, None, :], (GROUP, CACHE, HD)).reshape(GROUP * CACHE, HD)

        def attend(g):
            rows = pl.ds(pl.multiple_of(g * GROUP, GROUP), GROUP)
            crow = pl.ds(pl.multiple_of(g * GROUP * CACHE, GROUP * CACHE), GROUP * CACHE)
            q = jnp.concatenate([qs[h, rows, :] for h in range(QH)] + [qs[0, rows, :]], axis=0).astype(BF16)
            here = srow == spread(posb[rows, :])
            keys = jnp.where(here, spread(kn[rows, :]), kbuf[buf, crow, :].astype(F32)).astype(BF16)
            vals = jnp.where(here, spread(vn[rows, :]), vbuf[buf, crow, :].astype(F32)).astype(BF16)
            sc = lax.dot_general(q, keys, (((1,), (1,)), ((), ())), preferred_element_type=F32)
            sc = (sc * (HD ** -0.5)).reshape(QH + 1, GROUP, GROUP * CACHE)
            ok = (vis[rows, :] > 0.5)[None]
            sc = jnp.where(ok, sc, -1e30)
            e = jnp.exp(sc - jnp.max(sc, axis=-1, keepdims=True))
            prob = e * (1.0 / jnp.sum(e, axis=-1, keepdims=True))
            o = dot(prob.reshape((QH + 1) * GROUP, GROUP * CACHE).astype(BF16), vals)
            for h in range(QH):
                at[h, rows, :] = o[h * GROUP:(h + 1) * GROUP]

        def attend_some(gg, carry):
            for u in range(UNROLL):
                attend(gg * UNROLL + u)
            return carry

        lax.fori_loop(0, ROWS // GROUP // UNROLL, attend_some, 0)

        @pl.when(layer + 1 < LAYERS)
        def _():
            for cp in kv_copies(layer + 1):
                cp.start()

        for h in range(QH):
            ab[:, h * HD:(h + 1) * HD] = at[h].astype(BF16)

        for b in range(3):
            wait_slot(base + 4 + b, 256, DIM)
        wait_slot(base + 7, 128, DIM)

        def out_step(j, carry):
            cols = pl.ds(pl.multiple_of(j * 256, 256), 256)
            part = dot(ab[:, 768:896], ring[slot_of(base + 7), :128, cols])
            for b in range(3):
                part = part + dot(ab[:, b * 256:(b + 1) * 256], ring[slot_of(base + 4 + b), :, cols])
            stage_a(j, part)

            @pl.when(j >= 2)
            def _():
                stage_b(0, j - 2)

            return carry

        lax.fori_loop(0, CH, out_step, 0)
        for b in range(4):
            issue(base + 4 + b + SLOTS)
        stage_b(0, CH - 2)
        stage_b(0, CH - 1)

        ss[...] = jnp.zeros_like(ss)
        acc_g[...] = jnp.zeros_like(acc_g)
        acc_u[...] = jnp.zeros_like(acc_u)
        stage_c2(0, 0)

        def gu_step(i, carry):
            @pl.when(i + 1 < PAIRS)
            def _():
                stage_c2(0, i + 1)

            stage_d2(i)
            h0, h1 = take(2 * layer + 1, i)
            n = base + 8 + 4 * i
            for k, acc in ((0, acc_g), (2, acc_u)):
                wait_slot(n + k, 256, FF)
                wait_slot(n + k + 1, 256, FF)
                s0, s1 = slot_of(n + k), slot_of(n + k + 1)
                for c0, w in tiles(FF, 512):
                    acc[:, c0:c0 + w] += dot(h0, ring[s0, :, c0:c0 + w]) + dot(h1, ring[s1, :, c0:c0 + w])
                issue(n + k + SLOTS)
                issue(n + k + 1 + SLOTS)
            return carry

        lax.fori_loop(0, PAIRS, gu_step, 0)
        scale2 = row_scale()
        for c0, w in tiles(FF, 512):
            gate = acc_g[:, c0:c0 + w] * scale2
            up = acc_u[:, c0:c0 + w] * scale2
            act[:, c0:c0 + w] = (gate * jax.nn.sigmoid(gate) * up).astype(BF16)

        def down_step(j, carry):
            n = base + 36 + j
            s = slot_of(n)
            wait_slot(n, 256, FF)
            parts = [jnp.zeros((ROWS, 256), F32), jnp.zeros((ROWS, 256), F32)]
            for b in range(18):
                parts[b % 2] = parts[b % 2] + dot(act[:, b * 256:(b + 1) * 256], ring[s, :, b * 256:(b + 1) * 256])
            last = jnp.concatenate([ring[s, :128, 4608:4736], ring[s, 128:, 4608:4736]], axis=1)
            part = parts[0] + (parts[1] + dot(act[:, 4608:4736], last))
            stage_a(j, part)
            issue(n + SLOTS)

            @pl.when(j >= 2)
            def _():
                stage_b(1, j - 2)

            return carry

        lax.fori_loop(0, CH, down_step, 0)
        stage_b(1, CH - 2)
        stage_b(1, CH - 1)
        return carry

    lax.fori_loop(0, LAYERS, layer_body, 0)

    stage_c2(1, 0)

    def last_step(i, carry):
        @pl.when(i + 1 < PAIRS)
        def _():
            stage_c2(1, i + 1)

        stage_d2(i)
        for b in range(4):
            blk = 4 * i + b
            pltpu.make_async_copy(x.at[blk], out_hbm.at[:, pl.ds(pl.multiple_of(blk * 128, 128), 128)], x_sem).start()
        return carry

    lax.fori_loop(0, PAIRS, last_step, 0)
    pltpu.make_async_copy(x, x, x_sem).wait()


def fused_layers(x, positions, norm_attn, norm_mlp, wq, wk, wv, wo, wg, wu, wd, kc, vc):
    half = HD // 2
    freq = (np.float32(ROPE_BASE) ** (-np.arange(half, dtype=np.float32) / np.float32(half))).astype(np.float32)
    freq = jnp.asarray(np.concatenate([freq, freq])[None, :])
    vm = pl.BlockSpec(memory_space=pltpu.VMEM)
    hbm = pl.BlockSpec(memory_space=pl.ANY)
    vmem = pltpu.VMEM
    dma = pltpu.SemaphoreType.DMA
    scratch = [
        vmem((SLOTS, 256, FF), BF16), dma((SLOTS,)),
        vmem((BLKS, ROWS, 128), BF16), dma,
        vmem((2 * LAYERS, 8, DIM), F32),
        vmem((ROWS, HD), F32), vmem((ROWS, HD), F32), vmem((ROWS, HD), F32),
        vmem((ROWS, GROUP * CACHE), F32),
        vmem((ROWS, HD), F32),
        vmem((ROWS, QKV), F32), vmem((QH, ROWS, HD), F32),
        vmem((ROWS, HD), F32), vmem((ROWS, HD), F32),
        vmem((QH, ROWS, HD), F32), vmem((ROWS, QH * HD), BF16),
        vmem((ROWS, FF), F32), vmem((ROWS, FF), F32), vmem((ROWS, FF), BF16),
        vmem((2, ROWS * CACHE, HD), BF16), vmem((2, ROWS * CACHE, HD), BF16), dma((2, 2)),
        vmem((CH, ROWS, 128), F32),
        vmem((CH, ROWS, 128), BF16), vmem((CH, ROWS, 128), BF16),
        vmem((CH, ROWS, 128), BF16), vmem((2, CH, ROWS, 128), BF16),
        dma((CH,)), dma((CH,)), dma((CH,)), dma((2, CH)), dma((CH,)), dma((CH,)),
    ]
    new_rows = jax.ShapeDtypeStruct((LAYERS, ROWS, HD), BF16)
    return pl.pallas_call(
        kernel,
        out_shape=(jax.ShapeDtypeStruct((ROWS, DIM), BF16), new_rows, new_rows),
        in_specs=[hbm, vm, vm, vm, vm] + [hbm] * 9,
        out_specs=(hbm, vm, vm),
        scratch_shapes=scratch,
        compiler_params=pltpu.CompilerParams(collective_id=0, has_side_effects=True, vmem_limit_bytes=67043328),
        name="layers",
    )(x, positions, norm_attn, norm_mlp, freq, wq, wk, wv, wo, wg, wu, wd, kc, vc)


def solution(mesh):
    def local_step(hidden_in, positions, norm_attn, norm_mlp, w_query, w_key, w_value, w_out, w_gate, w_up, w_down, key_cache, value_cache):
        flat = (LAYERS, ROWS * CACHE, HD)
        hidden, k_new, v_new = fused_layers(
            hidden_in, positions[None, :], norm_attn, norm_mlp, w_query, w_key, w_value, w_out, w_gate, w_up, w_down,
            key_cache.reshape(flat), value_cache.reshape(flat))
        write_row = (jnp.arange(CACHE)[None, :] == positions[:, None])[None, :, :, None, None]
        key_out = jnp.where(write_row, k_new[:, :, None, None, :], key_cache)
        value_out = jnp.where(write_row, v_new[:, :, None, None, :], value_cache)
        return hidden, key_out, value_out

    row_spec = P("data", None)
    col_spec = P(None, None, "model")
    split_spec = P(None, "model", None)
    cache_spec = P(None, "data", None, "model", None)
    in_specs = (row_spec, P("data"), P(None, None), P(None, None), col_spec, col_spec, col_spec, split_spec, col_spec, col_spec, split_spec, cache_spec, cache_spec)
    out_specs = (row_spec, cache_spec, cache_spec)
    return jax.shard_map(local_step, mesh=mesh, in_specs=in_specs, out_specs=out_specs, check_vma=False)
```

```python
import functools

import jax
import jax.numpy as jnp
import numpy as np
from jax import lax
from jax.experimental import pallas as pl
from jax.experimental.pallas import tpu as pltpu
from jax.sharding import PartitionSpec as P

NORM_EPS = 1e-6
ROPE_BASE = 10000.0
MESH = pl.DeviceIdType.MESH
F32 = jnp.float32
BF16 = jnp.bfloat16

LAYERS = 3
ROWS = 128
DIM = 3584
HD = 128
QH = 7
CACHE = 32
FF = 4736
BLKS = DIM // 128
PAIRS = DIM // 512
QKV = (QH + 2) * HD
PER_LAYER = 2 + 2 + 2 * PAIRS + PAIRS
SLOTS = 8
DOWN = 2.0 ** -32
UP = 2.0 ** 32
GROUP = 8
GROUPS = ROWS // GROUP
QROWS = (QH + 1) * GROUP
KEYS = GROUP * CACHE


def kernel(x_hbm, pos_ref, na_ref, nm_ref, freq_ref, wq, wk, wv, wo, wg, wu, wd, kc_hbm, vc_hbm,
           out_hbm, kn_out, vn_out, mask_out,
           ring, ring_sem, x, x_sem, gn, posb, cos_t, sin_t, vis, ss, qkv, qs, kn, vn, sc, pr, at, ab, acc_g, acc_u, act,
           kbuf, vbuf, kv_sem, own, a_send, a_recv, b_send, b_recv, a_ss, a_rs, b_ss, b_rs, c_ss, c_rs):
    me = lax.axis_index("model")
    core = lax.rem(me, 2)
    partner = me + 1 - 2 * core
    peer = lax.rem(me + 2, 4)

    def slot_of(n):
        return lax.rem(n, SLOTS)

    def start(layer, r, src, rows, cols):
        s = slot_of(layer * PER_LAYER + r)
        pltpu.make_async_copy(src, ring.at[s, rows, cols], ring_sem.at[s]).start()

    def issue_qkv(layer, r):
        for t in range(4 if r == 0 else 3):
            rows = slice((4 * r + t) * 512, (4 * r + t + 1) * 512)
            base = t * QKV
            start(layer, r, wq.at[layer, rows, :], slice(None), slice(base, base + QH * HD))
            start(layer, r, wk.at[layer, rows, :], slice(None), slice(base + QH * HD, base + (QH + 1) * HD))
            start(layer, r, wv.at[layer, rows, :], slice(None), slice(base + (QH + 1) * HD, base + QKV))

    def issue_out(layer, r):
        if r == 0:
            start(layer, 2, wo.at[layer, 0:512, :], slice(None), slice(0, DIM))
        else:
            start(layer, 3, wo.at[layer, 512:896, :], slice(0, 384), slice(0, DIM))

    def issue_gu(layer, i, which):
        rows = pl.ds(i * 512 if isinstance(i, int) else pl.multiple_of(i * 512, 512), 512)
        src = wu if which else wg
        start(layer, 4 + 2 * i + which, src.at[layer, rows, :], slice(None), slice(None))

    def issue_down(layer, j):
        off = j * 512 if isinstance(j, int) else pl.multiple_of(j * 512, 512)
        for b in range(9):
            start(layer, 18 + j, wd.at[layer, b * 512:(b + 1) * 512, pl.ds(off, 512)], slice(None), slice(b * 512, (b + 1) * 512))
        for q in range(4):
            cols = pl.ds(off + q * 128 if isinstance(j, int) else pl.multiple_of(off + q * 128, 128), 128)
            start(layer, 18 + j, wd.at[layer, 4608:4736, cols], slice(q * 128, (q + 1) * 128), slice(4608, 4736))

    def wait_slot(n, rows, cols):
        s = slot_of(n)
        pltpu.make_async_copy(wg.at[0, :rows, :cols], ring.at[s, :rows, :cols], ring_sem.at[s]).wait()

    def kv_copies(layer):
        b = lax.rem(layer, 2)
        return (pltpu.make_async_copy(kc_hbm.at[layer], kbuf.at[b], kv_sem.at[0, b]),
                pltpu.make_async_copy(vc_hbm.at[layer], vbuf.at[b], kv_sem.at[1, b]))

    barrier = pltpu.get_barrier_semaphore()
    for other in (partner, peer):
        pl.semaphore_signal(barrier, inc=1, device_id={"model": other}, device_id_type=MESH)

    def load_x(b, carry):
        pltpu.make_async_copy(x_hbm.at[:, pl.ds(pl.multiple_of(b * 128, 128), 128)], x.at[b], x_sem).start()
        return carry

    lax.fori_loop(0, BLKS, load_x, 0)

    issue_qkv(0, 0)
    issue_qkv(0, 1)
    for cp in kv_copies(0):
        cp.start()
    issue_out(0, 0)
    issue_out(0, 1)
    for k in range(4):
        issue_gu(0, k // 2, k % 2)

    for layer in range(LAYERS):
        for which, ref in enumerate((na_ref, nm_ref)):
            row = ref[layer:layer + 1, :].astype(F32) * DOWN
            gn[2 * layer + which] = jnp.broadcast_to(row, (8, DIM))
    pos_row = jnp.broadcast_to(pos_ref[...].astype(F32), (ROWS, ROWS))
    ri = lax.broadcasted_iota(jnp.int32, (ROWS, ROWS), 0)
    ci = lax.broadcasted_iota(jnp.int32, (ROWS, ROWS), 1)
    pos_col = jnp.sum(jnp.where(ri == ci, pos_row, 0.0), axis=1, keepdims=True)
    pos_b = jnp.broadcast_to(pos_col, (ROWS, HD))
    posb[...] = pos_b
    angle = pos_b * freq_ref[...]
    cos_t[...] = jnp.cos(angle)
    sin_v = jnp.sin(angle)
    sin_t[...] = jnp.where(ci < HD // 2, -sin_v, sin_v)
    r2 = lax.broadcasted_iota(jnp.int32, (ROWS, GROUP * CACHE), 0)
    c2 = lax.broadcasted_iota(jnp.int32, (ROWS, GROUP * CACHE), 1)
    mine = (c2 // CACHE) == lax.rem(r2, GROUP)
    seen = lax.rem(c2, CACHE).astype(F32) <= jnp.broadcast_to(pos_col, (ROWS, GROUP * CACHE))
    vis[...] = jnp.where(mine & seen, 1.0, 0.0)
    cs = lax.broadcasted_iota(jnp.int32, (ROWS, CACHE), 1).astype(F32)
    mask_out[...] = jnp.where(cs == jnp.broadcast_to(pos_col, (ROWS, CACHE)), 1.0, 0.0)

    pltpu.make_async_copy(x, x, x_sem).wait()
    pl.semaphore_wait(barrier, 2)

    def a_copy(j):
        return pltpu.make_async_remote_copy(a_send.at[j], a_recv.at[j], a_ss.at[j], a_rs.at[j],
                                            device_id={"model": partner}, device_id_type=MESH)

    def b_copy(p, j):
        return pltpu.make_async_remote_copy(b_send.at[j], b_recv.at[p, j], b_ss.at[j], b_rs.at[p, j],
                                            device_id={"model": peer}, device_id_type=MESH)

    def c_copy(j, half):
        blk = pl.ds(4 * j + 2 * half, 2)
        return pltpu.make_async_remote_copy(x.at[blk], x.at[blk], c_ss.at[j], c_rs.at[j],
                                            device_id={"model": partner}, device_id_type=MESH)

    def stage_a(j, part):
        first = core == 0
        for t in range(2):
            lo, hi = part[:, t * 128:(t + 1) * 128], part[:, (t + 2) * 128:(t + 3) * 128]
            own[j, t] = jnp.where(first, lo, hi)
            a_send[j, t] = jnp.where(first, hi, lo).astype(BF16)
        a_copy(j).start()

    def stage_b(p, j):
        a_copy(j).wait_recv()
        b_send[j] = (own[j] + a_recv[j].astype(F32)).astype(BF16)
        b_copy(p, j).start()

    def stage_c(p, j):
        b_copy(p, j).wait_recv()
        total = b_send[j].astype(F32) + b_recv[p, j].astype(F32)
        blk = pl.ds(4 * j + 2 * core, 2)
        x[blk] = (x[blk].astype(F32) + total).astype(BF16)
        c_copy(j, core).start()
        a_copy(j).wait_send()
        b_copy(p, j).wait_send()

    def stage_d(j):
        c_copy(j, 1 - core).wait_recv()
        c_copy(j, core).wait_send()

    def take(row, i):
        outs = []
        sq = ss[...]
        for b in range(4):
            blk = x[4 * i + b].astype(F32)
            sq = sq + blk * blk
            off = i * 512 + b * 128 if isinstance(i, int) else pl.multiple_of(i * 512 + b * 128, 128)
            outs.append((blk * gn[row, 0:1, pl.ds(off, 128)]).astype(BF16))
        ss[...] = sq
        return jnp.concatenate(outs, axis=1)

    def row_scale():
        mean = jnp.sum(ss[...], axis=1, keepdims=True) * (1.0 / DIM)
        return lax.rsqrt(mean + NORM_EPS) * UP

    def dot(a, b):
        return jnp.dot(a, b, preferred_element_type=F32)

    def tiles(width, step):
        return [(n, min(step, width - n)) for n in range(0, width, step)]

    def layer_body(layer, carry):
        base = layer * PER_LAYER
        ss[...] = jnp.zeros_like(ss)
        qkv[...] = jnp.zeros_like(qkv)

        @pl.when(layer > 0)
        def _():
            stage_c(1, 0)

        def qkv_step(i, carry):
            @pl.when((layer > 0) & (i + 1 < PAIRS))
            def _():
                stage_c(1, i + 1)

            @pl.when(layer > 0)
            def _():
                stage_d(i)

            h = take(2 * layer, i)
            s = slot_of(base + i // 4)
            first = lax.rem(i, 4) * QKV
            for c0, w in tiles(QKV, 512):
                qkv[:, c0:c0 + w] += dot(h, ring[s, :, pl.ds(pl.multiple_of(first + c0, 128), w)])
            return carry

        wait_slot(base, 512, 4 * QKV)
        lax.fori_loop(0, 4, qkv_step, 0)
        issue_gu(layer, 2, 0)
        wait_slot(base + 1, 512, 3 * QKV)
        lax.fori_loop(4, PAIRS, qkv_step, 0)
        issue_gu(layer, 2, 1)

        scale = row_scale()
        cos_v, sin_v = cos_t[...], sin_t[...]

        def head(idx):
            return (qkv[:, idx * HD:(idx + 1) * HD] * scale).astype(BF16)

        def rotate(v):
            v = v.astype(F32)
            return (v * cos_v + pltpu.roll(v, HD // 2, axis=1) * sin_v).astype(BF16)

        for h in range(QH):
            qs[h] = rotate(head(h)).astype(F32)
        k_new = rotate(head(QH))
        v_new = head(QH + 1)
        kn[...] = k_new.astype(F32)
        vn[...] = v_new.astype(F32)
        kn_out[layer] = k_new
        vn_out[layer] = v_new
        for cp in kv_copies(layer):
            cp.wait()
        buf = lax.rem(layer, 2)
        srow = lax.rem(lax.broadcasted_iota(jnp.int32, (GROUP * CACHE, HD), 0), CACHE).astype(F32)

        def spread(v):
            return jnp.broadcast_to(v[:, None, :], (GROUP, CACHE, HD)).reshape(GROUP * CACHE, HD)

        span = [slice(g * GROUP, (g + 1) * GROUP) for g in range(GROUPS)]
        cspan = [slice(g * KEYS, (g + 1) * KEYS) for g in range(GROUPS)]
        for g in range(GROUPS):
            here = srow == spread(posb[span[g], :])
            kbuf[buf, cspan[g], :] = jnp.where(here, spread(kn[span[g], :]), kbuf[buf, cspan[g], :].astype(F32)).astype(BF16)
            vbuf[buf, cspan[g], :] = jnp.where(here, spread(vn[span[g], :]), vbuf[buf, cspan[g], :].astype(F32)).astype(BF16)
        for g in range(GROUPS):
            q = jnp.concatenate([qs[h, span[g], :] for h in range(QH)] + [qs[0, span[g], :]], axis=0).astype(BF16)
            sc[g] = lax.dot_general(q, kbuf[buf, cspan[g], :], (((1,), (1,)), ((), ())), preferred_element_type=F32)
        for g in range(GROUPS):
            raw = (sc[g] * (HD ** -0.5)).reshape(QH + 1, GROUP, KEYS)
            raw = jnp.where((vis[span[g], :] > 0.5)[None], raw, -1e30)
            e = jnp.exp(raw - jnp.max(raw, axis=-1, keepdims=True))
            prob = e * (1.0 / jnp.sum(e, axis=-1, keepdims=True))
            pr[g] = prob.reshape(QROWS, KEYS).astype(BF16)
        for g in range(GROUPS):
            o = dot(pr[g], vbuf[buf, cspan[g], :])
            for h in range(QH):
                at[h, span[g], :] = o[h * GROUP:(h + 1) * GROUP]

        @pl.when(layer + 1 < LAYERS)
        def _():
            for cp in kv_copies(layer + 1):
                cp.start()

        for h in range(QH):
            ab[:, h * HD:(h + 1) * HD] = at[h].astype(BF16)

        wait_slot(base + 2, 512, DIM)
        wait_slot(base + 3, 384, DIM)
        for j in range(PAIRS):
            cols = slice(j * 512, (j + 1) * 512)
            part = dot(ab[:, :512], ring[slot_of(base + 2), :, cols]) + dot(ab[:, 512:], ring[slot_of(base + 3), :384, cols])
            stage_a(j, part)
            if j >= 3:
                stage_b(0, j - 3)
        issue_gu(layer, 3, 0)
        issue_gu(layer, 3, 1)
        for j in range(PAIRS - 3, PAIRS):
            stage_b(0, j)

        ss[...] = jnp.zeros_like(ss)
        stage_c(0, 0)

        def gu_step(i, issue, first=False, last=False):
            if not last:
                stage_c(0, i + 1)
            stage_d(i)
            h = take(2 * layer + 1, i)
            n = base + 4 + 2 * i
            for k, acc in ((0, acc_g), (1, acc_u)):
                wait_slot(n + k, 512, FF)
                s = slot_of(n + k)
                for c0, w in tiles(FF, 512):
                    part = dot(h, ring[s, :, c0:c0 + w])
                    if first:
                        acc[:, c0:c0 + w] = part
                    else:
                        acc[:, c0:c0 + w] += part
                issue(k)

        gu_step(0, lambda k: issue_gu(layer, 4, k), first=True)

        def gu_low(i, carry):
            gu_step(i, lambda k: issue_gu(layer, i + 4, k))
            return carry

        def gu_high(i, carry):
            gu_step(i, lambda k: issue_down(layer, 2 * (i - 3) + k))
            return carry

        lax.fori_loop(1, 3, gu_low, 0)
        lax.fori_loop(3, 6, gu_high, 0)

        def issue_last(k):
            if k == 0:
                issue_down(layer, 6)
            else:
                @pl.when(layer + 1 < LAYERS)
                def _():
                    issue_qkv(layer + 1, 0)

        gu_step(6, issue_last, last=True)
        scale2 = row_scale()
        for c0, w in tiles(FF, 512):
            gate = acc_g[:, c0:c0 + w] * scale2
            up = acc_u[:, c0:c0 + w] * scale2
            act[:, c0:c0 + w] = (gate * jax.nn.sigmoid(gate) * up).astype(BF16)

        def down_step(j, issue, lead):
            n = base + 18 + j
            s = slot_of(n)
            wait_slot(n, 512, FF)
            part = dot(act[:, :512], ring[s, :, :512])
            for b in range(1, 9):
                part = part + dot(act[:, b * 512:(b + 1) * 512], ring[s, :, b * 512:(b + 1) * 512])
            last = jnp.concatenate([ring[s, q * 128:(q + 1) * 128, 4608:4736] for q in range(4)], axis=1)
            part = part + dot(act[:, 4608:4736], last)
            stage_a(j, part)

            @pl.when(layer + 1 < LAYERS)
            def _():
                issue()

            if lead:
                stage_b(1, j - 1)

        down_step(0, lambda: issue_qkv(layer + 1, 1), False)
        down_step(1, lambda: issue_out(layer + 1, 0), True)
        down_step(2, lambda: issue_out(layer + 1, 1), True)

        def down_even(t, carry):
            down_step(3 + 2 * t, lambda: issue_gu(layer + 1, t, 0), True)
            down_step(4 + 2 * t, lambda: issue_gu(layer + 1, t, 1), True)
            return carry

        lax.fori_loop(0, 2, down_even, 0)
        stage_b(1, PAIRS - 1)
        return carry

    lax.fori_loop(0, LAYERS, layer_body, 0)

    stage_c(1, 0)

    def last_step(i, carry):
        @pl.when(i + 1 < PAIRS)
        def _():
            stage_c(1, i + 1)

        stage_d(i)
        for b in range(4):
            blk = 4 * i + b
            pltpu.make_async_copy(x.at[blk], out_hbm.at[:, pl.ds(pl.multiple_of(blk * 128, 128), 128)], x_sem).start()
        return carry

    lax.fori_loop(0, PAIRS, last_step, 0)
    pltpu.make_async_copy(x, x, x_sem).wait()


def fused_layers(x, positions, norm_attn, norm_mlp, wq, wk, wv, wo, wg, wu, wd, kc, vc):
    half = HD // 2
    freq = (np.float32(ROPE_BASE) ** (-np.arange(half, dtype=np.float32) / np.float32(half))).astype(np.float32)
    freq = jnp.asarray(np.concatenate([freq, freq])[None, :])
    vm = pl.BlockSpec(memory_space=pltpu.VMEM)
    hbm = pl.BlockSpec(memory_space=pl.ANY)
    vmem = pltpu.VMEM
    dma = pltpu.SemaphoreType.DMA
    scratch = [
        vmem((SLOTS, 512, FF), BF16), dma((SLOTS,)),
        vmem((BLKS, ROWS, 128), BF16), dma,
        vmem((2 * LAYERS, 8, DIM), F32),
        vmem((ROWS, HD), F32), vmem((ROWS, HD), F32), vmem((ROWS, HD), F32),
        vmem((ROWS, GROUP * CACHE), F32),
        vmem((ROWS, HD), F32),
        vmem((ROWS, QKV), F32), vmem((QH, ROWS, HD), F32),
        vmem((ROWS, HD), F32), vmem((ROWS, HD), F32),
        vmem((GROUPS, QROWS, KEYS), F32), vmem((GROUPS, QROWS, KEYS), BF16),
        vmem((QH, ROWS, HD), F32), vmem((ROWS, QH * HD), BF16),
        vmem((ROWS, FF), F32), vmem((ROWS, FF), F32), vmem((ROWS, FF), BF16),
        vmem((2, ROWS * CACHE, HD), BF16), vmem((2, ROWS * CACHE, HD), BF16), dma((2, 2)),
        vmem((PAIRS, 2, ROWS, 128), F32),
        vmem((PAIRS, 2, ROWS, 128), BF16), vmem((PAIRS, 2, ROWS, 128), BF16),
        vmem((PAIRS, 2, ROWS, 128), BF16), vmem((2, PAIRS, 2, ROWS, 128), BF16),
        dma((PAIRS,)), dma((PAIRS,)), dma((PAIRS,)), dma((2, PAIRS)), dma((PAIRS,)), dma((PAIRS,)),
    ]
    new_rows = jax.ShapeDtypeStruct((LAYERS, ROWS, HD), BF16)
    return pl.pallas_call(
        kernel,
        out_shape=(jax.ShapeDtypeStruct((ROWS, DIM), BF16), new_rows, new_rows, jax.ShapeDtypeStruct((ROWS, CACHE), F32)),
        in_specs=[hbm, vm, vm, vm, vm] + [hbm] * 9,
        out_specs=(hbm, vm, vm, vm),
        scratch_shapes=scratch,
        compiler_params=pltpu.CompilerParams(collective_id=0, has_side_effects=True, vmem_limit_bytes=67043328),
        name="layers",
    )(x, positions, norm_attn, norm_mlp, freq, wq, wk, wv, wo, wg, wu, wd, kc, vc)


def solution(mesh):
    def local_step(hidden_in, positions, norm_attn, norm_mlp, w_query, w_key, w_value, w_out, w_gate, w_up, w_down, key_cache, value_cache):
        flat = (LAYERS, ROWS * CACHE, HD)
        hidden, k_new, v_new, mask = fused_layers(
            hidden_in, positions[None, :], norm_attn, norm_mlp, w_query, w_key, w_value, w_out, w_gate, w_up, w_down,
            key_cache.reshape(flat), value_cache.reshape(flat))
        write_row = (mask > 0.5)[None, :, :, None, None]
        key_out = jnp.where(write_row, k_new[:, :, None, None, :], key_cache)
        value_out = jnp.where(write_row, v_new[:, :, None, None, :], value_cache)
        return hidden, key_out, value_out

    row_spec = P("data", None)
    col_spec = P(None, None, "model")
    split_spec = P(None, "model", None)
    cache_spec = P(None, "data", None, "model", None)
    in_specs = (row_spec, P("data"), P(None, None), P(None, None), col_spec, col_spec, col_spec, split_spec, col_spec, col_spec, split_spec, cache_spec, cache_spec)
    out_specs = (row_spec, cache_spec, cache_spec)
    return jax.shard_map(local_step, mesh=mesh, in_specs=in_specs, out_specs=out_specs, check_vma=False)
```

```python
import functools

import jax
import jax.numpy as jnp
import numpy as np
from jax import lax
from jax.experimental import pallas as pl
from jax.experimental.pallas import tpu as pltpu
from jax.sharding import PartitionSpec as P

NORM_EPS = 1e-6
ROPE_BASE = 10000.0
MESH = pl.DeviceIdType.MESH
F32 = jnp.float32
BF16 = jnp.bfloat16

LAYERS = 3
ROWS = 128
DIM = 3584
HD = 128
QH = 7
CACHE = 32
FF = 4736
BLKS = DIM // 128
PAIRS = DIM // 512
QKV = (QH + 2) * HD
PER_LAYER = 2 + 2 + 2 * PAIRS + PAIRS
SLOTS = 10
DOWN = 2.0 ** -32
UP = 2.0 ** 32
GROUP = 8
GROUPS = ROWS // GROUP
QROWS = (QH + 1) * GROUP
KEYS = GROUP * CACHE


def kernel(x_hbm, pos_ref, na_ref, nm_ref, freq_ref, wq, wk, wv, wo, wg, wu, wd, kc_hbm, vc_hbm,
           out_hbm, kn_out, vn_out, mask_out,
           ring, ring_sem, x, x_sem, gn, posb, cos_t, sin_t, vis, ss, kn, vn, ab, acc_g, acc_u, act,
           kbuf, vbuf, kv_sem, own, a_send, a_recv, b_send, b_recv, a_ss, a_rs, b_ss, b_rs, c_ss, c_rs):
    me = lax.axis_index("model")
    core = lax.rem(me, 2)
    partner = me + 1 - 2 * core
    peer = lax.rem(me + 2, 4)

    at = [acc_u.at[:, h * HD:(h + 1) * HD] for h in range(QH)]
    qs = [acc_u.at[:, (QH + h) * HD:(QH + h + 1) * HD] for h in range(QH)]
    qkv = acc_u.at[:, 2 * QH * HD:2 * QH * HD + QKV]
    sc = [acc_g.at[:QROWS, g * KEYS:(g + 1) * KEYS] for g in range(GROUPS)]
    pr = [act.at[:QROWS, g * KEYS:(g + 1) * KEYS] for g in range(GROUPS)]

    def slot_of(n):
        return lax.rem(n, SLOTS)

    def start(layer, r, src, rows, cols):
        s = slot_of(layer * PER_LAYER + r)
        pltpu.make_async_copy(src, ring.at[s, rows, cols], ring_sem.at[s]).start()

    def issue_qkv(layer, r):
        for t in range(4 if r == 0 else 3):
            rows = slice((4 * r + t) * 512, (4 * r + t + 1) * 512)
            base = t * QKV
            start(layer, r, wq.at[layer, rows, :], slice(None), slice(base, base + QH * HD))
            start(layer, r, wk.at[layer, rows, :], slice(None), slice(base + QH * HD, base + (QH + 1) * HD))
            start(layer, r, wv.at[layer, rows, :], slice(None), slice(base + (QH + 1) * HD, base + QKV))

    def issue_out(layer, r):
        if r == 0:
            start(layer, 2, wo.at[layer, 0:512, :], slice(None), slice(0, DIM))
        else:
            start(layer, 3, wo.at[layer, 512:896, :], slice(0, 384), slice(0, DIM))

    def issue_gu(layer, i, which):
        rows = pl.ds(i * 512 if isinstance(i, int) else pl.multiple_of(i * 512, 512), 512)
        src = wu if which else wg
        start(layer, 4 + 2 * i + which, src.at[layer, rows, :], slice(None), slice(None))

    def issue_down(layer, j):
        off = j * 512 if isinstance(j, int) else pl.multiple_of(j * 512, 512)
        for b in range(9):
            start(layer, 18 + j, wd.at[layer, b * 512:(b + 1) * 512, pl.ds(off, 512)], slice(None), slice(b * 512, (b + 1) * 512))
        for q in range(4):
            cols = pl.ds(off + q * 128 if isinstance(j, int) else pl.multiple_of(off + q * 128, 128), 128)
            start(layer, 18 + j, wd.at[layer, 4608:4736, cols], slice(q * 128, (q + 1) * 128), slice(4608, 4736))

    def wait_slot(n, rows, cols):
        s = slot_of(n)
        pltpu.make_async_copy(wg.at[0, :rows, :cols], ring.at[s, :rows, :cols], ring_sem.at[s]).wait()

    def kv_copies(layer):
        return (pltpu.make_async_copy(kc_hbm.at[layer], kbuf, kv_sem.at[0]),
                pltpu.make_async_copy(vc_hbm.at[layer], vbuf, kv_sem.at[1]))

    barrier = pltpu.get_barrier_semaphore()
    for other in (partner, peer):
        pl.semaphore_signal(barrier, inc=1, device_id={"model": other}, device_id_type=MESH)

    def load_x(b, carry):
        pltpu.make_async_copy(x_hbm.at[:, pl.ds(pl.multiple_of(b * 128, 128), 128)], x.at[b], x_sem).start()
        return carry

    lax.fori_loop(0, BLKS, load_x, 0)

    issue_qkv(0, 0)
    issue_qkv(0, 1)
    for cp in kv_copies(0):
        cp.start()
    issue_out(0, 0)
    issue_out(0, 1)
    for k in range(6):
        issue_gu(0, k // 2, k % 2)

    for layer in range(LAYERS):
        for which, ref in enumerate((na_ref, nm_ref)):
            row = ref[layer:layer + 1, :].astype(F32) * DOWN
            for blk in range(BLKS):
                gn[2 * layer + which, blk // 4, blk % 4:blk % 4 + 1, :] = row[:, blk * 128:(blk + 1) * 128]
    pos_row = jnp.broadcast_to(pos_ref[...].astype(F32), (ROWS, ROWS))
    ri = lax.broadcasted_iota(jnp.int32, (ROWS, ROWS), 0)
    ci = lax.broadcasted_iota(jnp.int32, (ROWS, ROWS), 1)
    pos_col = jnp.sum(jnp.where(ri == ci, pos_row, 0.0), axis=1, keepdims=True)
    pos_b = jnp.broadcast_to(pos_col, (ROWS, HD))
    posb[...] = pos_b
    angle = pos_b * freq_ref[...]
    cos_t[...] = jnp.cos(angle)
    sin_v = jnp.sin(angle)
    sin_t[...] = jnp.where(ci < HD // 2, -sin_v, sin_v)
    r2 = lax.broadcasted_iota(jnp.int32, (ROWS, GROUP * CACHE), 0)
    c2 = lax.broadcasted_iota(jnp.int32, (ROWS, GROUP * CACHE), 1)
    mine = (c2 // CACHE) == lax.rem(r2, GROUP)
    seen = lax.rem(c2, CACHE).astype(F32) <= jnp.broadcast_to(pos_col, (ROWS, GROUP * CACHE))
    vis[...] = jnp.where(mine & seen, 1.0, 0.0)
    cs = lax.broadcasted_iota(jnp.int32, (ROWS, CACHE), 1).astype(F32)
    mask_out[...] = jnp.where(cs == jnp.broadcast_to(pos_col, (ROWS, CACHE)), 1.0, 0.0)

    pltpu.make_async_copy(x, x, x_sem).wait()
    pl.semaphore_wait(barrier, 2)

    def a_copy(j):
        return pltpu.make_async_remote_copy(a_send.at[j], a_recv.at[j], a_ss.at[j], a_rs.at[j],
                                            device_id={"model": partner}, device_id_type=MESH)

    def b_copy(p, j):
        return pltpu.make_async_remote_copy(b_send.at[j], b_recv.at[p, j], b_ss.at[j], b_rs.at[p, j],
                                            device_id={"model": peer}, device_id_type=MESH)

    def c_copy(j, half):
        blk = pl.ds(4 * j + 2 * half, 2)
        return pltpu.make_async_remote_copy(x.at[blk], x.at[blk], c_ss.at[j], c_rs.at[j],
                                            device_id={"model": partner}, device_id_type=MESH)

    def stage_a(j, part):
        first = core == 0
        for t in range(2):
            lo, hi = part[:, t * 128:(t + 1) * 128], part[:, (t + 2) * 128:(t + 3) * 128]
            own[j, t] = jnp.where(first, lo, hi)
            a_send[j, t] = jnp.where(first, hi, lo).astype(BF16)
        a_copy(j).start()

    def stage_b(p, j):
        a_copy(j).wait_recv()
        b_send[j] = (own[j] + a_recv[j].astype(F32)).astype(BF16)
        b_copy(p, j).start()

    def stage_c(p, j):
        b_copy(p, j).wait_recv()
        total = b_send[j].astype(F32) + b_recv[p, j].astype(F32)
        blk = pl.ds(4 * j + 2 * core, 2)
        x[blk] = (x[blk].astype(F32) + total).astype(BF16)
        c_copy(j, core).start()
        a_copy(j).wait_send()
        b_copy(p, j).wait_send()

    def stage_d(j):
        c_copy(j, 1 - core).wait_recv()
        c_copy(j, core).wait_send()

    def take(row, i):
        outs = []
        sq = ss[...]
        gains = gn[row, i]
        for b in range(4):
            blk = x[4 * i + b].astype(F32)
            sq = sq + blk * blk
            outs.append((blk * gains[b:b + 1, :]).astype(BF16))
        ss[...] = sq
        return jnp.concatenate(outs, axis=1)

    def row_scale():
        mean = jnp.sum(ss[...], axis=1, keepdims=True) * (1.0 / DIM)
        return lax.rsqrt(mean + NORM_EPS) * UP

    def dot(a, b):
        return jnp.dot(a, b, preferred_element_type=F32)

    def tiles(width, step):
        return [(n, min(step, width - n)) for n in range(0, width, step)]

    def layer_body(layer, carry):
        base = layer * PER_LAYER
        ss[...] = jnp.zeros_like(ss)
        qkv[...] = jnp.zeros((ROWS, QKV), F32)

        @pl.when(layer > 0)
        def _():
            stage_c(1, 0)

        def qkv_step(i, carry):
            @pl.when((layer > 0) & (i + 1 < PAIRS))
            def _():
                stage_c(1, i + 1)

            @pl.when(layer > 0)
            def _():
                stage_d(i)

            h = take(2 * layer, i)
            s = slot_of(base + i // 4)
            first = lax.rem(i, 4) * QKV
            for c0, w in tiles(QKV, 512):
                qkv[:, c0:c0 + w] += dot(h, ring[s, :, pl.ds(pl.multiple_of(first + c0, 128), w)])
            return carry

        wait_slot(base, 512, 4 * QKV)
        lax.fori_loop(0, 4, qkv_step, 0)
        issue_gu(layer, 3, 0)
        wait_slot(base + 1, 512, 3 * QKV)
        lax.fori_loop(4, PAIRS, qkv_step, 0)
        issue_gu(layer, 3, 1)

        scale = row_scale()
        cos_v, sin_v = cos_t[...], sin_t[...]

        def head(idx):
            return (qkv[:, idx * HD:(idx + 1) * HD] * scale).astype(BF16)

        def rotate(v):
            v = v.astype(F32)
            return (v * cos_v + pltpu.roll(v, HD // 2, axis=1) * sin_v).astype(BF16)

        for h in range(QH):
            qs[h][...] = rotate(head(h)).astype(F32)
        k_new = rotate(head(QH))
        v_new = head(QH + 1)
        kn[...] = k_new.astype(F32)
        vn[...] = v_new.astype(F32)
        kn_out[layer] = k_new
        vn_out[layer] = v_new
        for cp in kv_copies(layer):
            cp.wait()
        wait_slot(base + 2, 512, DIM)
        wait_slot(base + 3, 384, DIM)
        srow = lax.rem(lax.broadcasted_iota(jnp.int32, (GROUP * CACHE, HD), 0), CACHE).astype(F32)

        def spread(v):
            return jnp.broadcast_to(v[:, None, :], (GROUP, CACHE, HD)).reshape(GROUP * CACHE, HD)

        span = [slice(g * GROUP, (g + 1) * GROUP) for g in range(GROUPS)]
        cspan = [slice(g * KEYS, (g + 1) * KEYS) for g in range(GROUPS)]
        for g in range(GROUPS):
            here = srow == spread(posb[span[g], :])
            kbuf[cspan[g], :] = jnp.where(here, spread(kn[span[g], :]), kbuf[cspan[g], :].astype(F32)).astype(BF16)
            vbuf[cspan[g], :] = jnp.where(here, spread(vn[span[g], :]), vbuf[cspan[g], :].astype(F32)).astype(BF16)
        for g in range(GROUPS):
            q = jnp.concatenate([qs[h][span[g], :] for h in range(QH)] + [qs[0][span[g], :]], axis=0).astype(BF16)
            sc[g][...] = lax.dot_general(q, kbuf[cspan[g], :], (((1,), (1,)), ((), ())), preferred_element_type=F32)
        for g in range(GROUPS):
            raw = (sc[g][...] * (HD ** -0.5)).reshape(QH + 1, GROUP, KEYS)
            raw = jnp.where((vis[span[g], :] > 0.5)[None], raw, -1e30)
            e = jnp.exp(raw - jnp.max(raw, axis=-1, keepdims=True))
            prob = e * (1.0 / jnp.sum(e, axis=-1, keepdims=True))
            pr[g][...] = prob.reshape(QROWS, KEYS).astype(BF16)
        for g in range(GROUPS):
            o = dot(pr[g][...], vbuf[cspan[g], :])
            for h in range(QH):
                at[h][span[g], :] = o[h * GROUP:(h + 1) * GROUP]

        @pl.when(layer + 1 < LAYERS)
        def _():
            for cp in kv_copies(layer + 1):
                cp.start()

        for h in range(QH):
            ab[:, h * HD:(h + 1) * HD] = at[h][...].astype(BF16)

        for j in range(PAIRS):
            cols = slice(j * 512, (j + 1) * 512)
            part = dot(ab[:, :512], ring[slot_of(base + 2), :, cols]) + dot(ab[:, 512:], ring[slot_of(base + 3), :384, cols])
            stage_a(j, part)
            if j >= 3:
                stage_b(0, j - 3)
        issue_gu(layer, 4, 0)
        issue_gu(layer, 4, 1)
        for j in range(PAIRS - 3, PAIRS):
            stage_b(0, j)

        ss[...] = jnp.zeros_like(ss)
        stage_c(0, 0)

        def gu_step(i, issue, first=False, last=False):
            if not last:
                stage_c(0, i + 1)
            stage_d(i)
            h = take(2 * layer + 1, i)
            n = base + 4 + 2 * i
            for k, acc in ((0, acc_g), (1, acc_u)):
                wait_slot(n + k, 512, FF)
                s = slot_of(n + k)
                for c0, w in tiles(FF, 512):
                    part = dot(h, ring[s, :, c0:c0 + w])
                    if first:
                        acc[:, c0:c0 + w] = part
                    else:
                        acc[:, c0:c0 + w] += part
                issue(k)

        gu_step(0, lambda k: issue_gu(layer, 5, k), first=True)
        gu_step(1, lambda k: issue_gu(layer, 6, k))

        def gu_mid(i, carry):
            gu_step(i, lambda k: issue_down(layer, 2 * (i - 2) + k))
            return carry

        lax.fori_loop(2, 5, gu_mid, 0)

        def more(fn):
            pl.when(layer + 1 < LAYERS)(fn)

        gu_step(5, lambda k: more(lambda: issue_qkv(layer + 1, 0)) if k else issue_down(layer, 6))
        gu_step(6, lambda k: more(lambda: issue_out(layer + 1, 0)) if k else more(lambda: issue_qkv(layer + 1, 1)), last=True)
        wait_slot(base + 18, 512, FF)
        scale2 = row_scale()
        for c0, w in tiles(FF, 512):
            gate = acc_g[:, c0:c0 + w] * scale2
            up = acc_u[:, c0:c0 + w] * scale2
            act[:, c0:c0 + w] = (gate * jax.nn.sigmoid(gate) * up).astype(BF16)

        def down_step(j, issue, lead):
            n = base + 18 + j
            s = slot_of(n)
            if lead:
                wait_slot(n, 512, FF)
            part = dot(act[:, :512], ring[s, :, :512])
            for b in range(1, 9):
                part = part + dot(act[:, b * 512:(b + 1) * 512], ring[s, :, b * 512:(b + 1) * 512])
            last = jnp.concatenate([ring[s, q * 128:(q + 1) * 128, 4608:4736] for q in range(4)], axis=1)
            part = part + dot(act[:, 4608:4736], last)
            stage_a(j, part)

            @pl.when(layer + 1 < LAYERS)
            def _():
                issue()

            if lead:
                stage_b(1, j - 1)

        down_step(0, lambda: issue_out(layer + 1, 1), False)

        def down_pair(t, carry):
            down_step(1 + 2 * t, lambda: issue_gu(layer + 1, t, 0), True)
            down_step(2 + 2 * t, lambda: issue_gu(layer + 1, t, 1), True)
            return carry

        lax.fori_loop(0, 3, down_pair, 0)
        stage_b(1, PAIRS - 1)
        return carry

    lax.fori_loop(0, LAYERS, layer_body, 0)

    stage_c(1, 0)

    def last_step(i, carry):
        @pl.when(i + 1 < PAIRS)
        def _():
            stage_c(1, i + 1)

        stage_d(i)
        for b in range(4):
            blk = 4 * i + b
            pltpu.make_async_copy(x.at[blk], out_hbm.at[:, pl.ds(pl.multiple_of(blk * 128, 128), 128)], x_sem).start()
        return carry

    lax.fori_loop(0, PAIRS, last_step, 0)
    pltpu.make_async_copy(x, x, x_sem).wait()


def fused_layers(x, positions, norm_attn, norm_mlp, wq, wk, wv, wo, wg, wu, wd, kc, vc):
    half = HD // 2
    freq = (np.float32(ROPE_BASE) ** (-np.arange(half, dtype=np.float32) / np.float32(half))).astype(np.float32)
    freq = jnp.asarray(np.concatenate([freq, freq])[None, :])
    vm = pl.BlockSpec(memory_space=pltpu.VMEM)
    hbm = pl.BlockSpec(memory_space=pl.ANY)
    vmem = pltpu.VMEM
    dma = pltpu.SemaphoreType.DMA
    scratch = [
        vmem((SLOTS, 512, FF), BF16), dma((SLOTS,)),
        vmem((BLKS, ROWS, 128), BF16), dma,
        vmem((2 * LAYERS, PAIRS, 8, 128), F32),
        vmem((ROWS, HD), F32), vmem((ROWS, HD), F32), vmem((ROWS, HD), F32),
        vmem((ROWS, GROUP * CACHE), F32),
        vmem((ROWS, HD), F32),
        vmem((ROWS, HD), F32), vmem((ROWS, HD), F32), vmem((ROWS, QH * HD), BF16),
        vmem((ROWS, FF), F32), vmem((ROWS, FF), F32), vmem((ROWS, FF), BF16),
        vmem((ROWS * CACHE, HD), BF16), vmem((ROWS * CACHE, HD), BF16), dma((2,)),
        vmem((PAIRS, 2, ROWS, 128), F32),
        vmem((PAIRS, 2, ROWS, 128), BF16), vmem((PAIRS, 2, ROWS, 128), BF16),
        vmem((PAIRS, 2, ROWS, 128), BF16), vmem((2, PAIRS, 2, ROWS, 128), BF16),
        dma((PAIRS,)), dma((PAIRS,)), dma((PAIRS,)), dma((2, PAIRS)), dma((PAIRS,)), dma((PAIRS,)),
    ]
    new_rows = jax.ShapeDtypeStruct((LAYERS, ROWS, HD), BF16)
    return pl.pallas_call(
        kernel,
        out_shape=(jax.ShapeDtypeStruct((ROWS, DIM), BF16), new_rows, new_rows, jax.ShapeDtypeStruct((ROWS, CACHE), F32)),
        in_specs=[hbm, vm, vm, vm, vm] + [hbm] * 9,
        out_specs=(hbm, vm, vm, vm),
        scratch_shapes=scratch,
        compiler_params=pltpu.CompilerParams(collective_id=0, has_side_effects=True, vmem_limit_bytes=67043328),
        name="layers",
    )(x, positions, norm_attn, norm_mlp, freq, wq, wk, wv, wo, wg, wu, wd, kc, vc)


def solution(mesh):
    def local_step(hidden_in, positions, norm_attn, norm_mlp, w_query, w_key, w_value, w_out, w_gate, w_up, w_down, key_cache, value_cache):
        flat = (LAYERS, ROWS * CACHE, HD)
        hidden, k_new, v_new, mask = fused_layers(
            hidden_in, positions[None, :], norm_attn, norm_mlp, w_query, w_key, w_value, w_out, w_gate, w_up, w_down,
            key_cache.reshape(flat), value_cache.reshape(flat))
        write_row = (mask > 0.5)[None, :, :, None, None]
        key_out = jnp.where(write_row, k_new[:, :, None, None, :], key_cache)
        value_out = jnp.where(write_row, v_new[:, :, None, None, :], value_cache)
        return hidden, key_out, value_out

    row_spec = P("data", None)
    col_spec = P(None, None, "model")
    split_spec = P(None, "model", None)
    cache_spec = P(None, "data", None, "model", None)
    in_specs = (row_spec, P("data"), P(None, None), P(None, None), col_spec, col_spec, col_spec, split_spec, col_spec, col_spec, split_spec, cache_spec, cache_spec)
    out_specs = (row_spec, cache_spec, cache_spec)
    return jax.shard_map(local_step, mesh=mesh, in_specs=in_specs, out_specs=out_specs, check_vma=False)
```

```python
import functools

import jax
import jax.numpy as jnp
import numpy as np
from jax import lax
from jax.experimental import pallas as pl
from jax.experimental.pallas import tpu as pltpu
from jax.sharding import PartitionSpec as P

NORM_EPS = 1e-6
ROPE_BASE = 10000.0
MESH = pl.DeviceIdType.MESH
F32 = jnp.float32
BF16 = jnp.bfloat16

LAYERS = 3
ROWS = 128
DIM = 3584
HD = 128
QH = 7
CACHE = 32
FF = 4736
BLKS = DIM // 128
PAIRS = DIM // 512
QKV = (QH + 2) * HD
PER_LAYER = 2 + 2 + 2 * PAIRS + PAIRS
SLOTS = 10
DOWN = 2.0 ** -32
UP = 2.0 ** 32
GROUP = 8
GROUPS = ROWS // GROUP
QROWS = (QH + 1) * GROUP
KEYS = GROUP * CACHE


def kernel(x_hbm, pos_hbm, na_hbm, nm_hbm, freq_hbm, wq, wk, wv, wo, wg, wu, wd, kc_hbm, vc_hbm,
           out_hbm, kn_out, vn_out, mask_out,
           pos_ref, na_ref, nm_ref, freq_ref, small_sem, kn16, vn16, mask16, row_sem,
           ring, ring_sem, x, x_sem, gn, posb, cos_t, sin_t, vis, ss, kn, vn, ab, acc_g, acc_u, act,
           kbuf, vbuf, kv_sem, own, a_send, a_recv, b_send, b_recv, a_ss, a_rs, b_ss, b_rs, c_ss, c_rs):
    me = lax.axis_index("model")
    core = lax.rem(me, 2)
    partner = me + 1 - 2 * core
    peer = lax.rem(me + 2, 4)

    at = [acc_u.at[:, h * HD:(h + 1) * HD] for h in range(QH)]
    qs = [acc_u.at[:, (QH + h) * HD:(QH + h + 1) * HD] for h in range(QH)]
    qkv = acc_u.at[:, 2 * QH * HD:2 * QH * HD + QKV]
    sc = [acc_g.at[:QROWS, g * KEYS:(g + 1) * KEYS] for g in range(GROUPS)]
    pr = [act.at[:QROWS, g * KEYS:(g + 1) * KEYS] for g in range(GROUPS)]

    def slot_of(n):
        return lax.rem(n, SLOTS)

    def start(layer, r, src, rows, cols):
        s = slot_of(layer * PER_LAYER + r)
        pltpu.make_async_copy(src, ring.at[s, rows, cols], ring_sem.at[s]).start(priority=1)

    def issue_qkv(layer, r):
        for t in range(4 if r == 0 else 3):
            rows = slice((4 * r + t) * 512, (4 * r + t + 1) * 512)
            base = t * QKV
            start(layer, r, wq.at[layer, rows, :], slice(None), slice(base, base + QH * HD))
            start(layer, r, wk.at[layer, rows, :], slice(None), slice(base + QH * HD, base + (QH + 1) * HD))
            start(layer, r, wv.at[layer, rows, :], slice(None), slice(base + (QH + 1) * HD, base + QKV))

    def issue_out(layer, r):
        if r == 0:
            start(layer, 2, wo.at[layer, 0:512, :], slice(None), slice(0, DIM))
        else:
            start(layer, 3, wo.at[layer, 512:896, :], slice(0, 384), slice(0, DIM))

    def issue_gu(layer, i, which):
        rows = pl.ds(i * 512 if isinstance(i, int) else pl.multiple_of(i * 512, 512), 512)
        src = wu if which else wg
        start(layer, 4 + 2 * i + which, src.at[layer, rows, :], slice(None), slice(None))

    def issue_down(layer, j):
        off = j * 512 if isinstance(j, int) else pl.multiple_of(j * 512, 512)
        for b in range(9):
            start(layer, 18 + j, wd.at[layer, b * 512:(b + 1) * 512, pl.ds(off, 512)], slice(None), slice(b * 512, (b + 1) * 512))
        for q in range(4):
            cols = pl.ds(off + q * 128 if isinstance(j, int) else pl.multiple_of(off + q * 128, 128), 128)
            start(layer, 18 + j, wd.at[layer, 4608:4736, cols], slice(q * 128, (q + 1) * 128), slice(4608, 4736))

    def wait_slot(n, rows, cols):
        s = slot_of(n)
        pltpu.make_async_copy(wg.at[0, :rows, :cols], ring.at[s, :rows, :cols], ring_sem.at[s]).wait()

    def kv_copies(layer):
        return (pltpu.make_async_copy(kc_hbm.at[layer], kbuf, kv_sem.at[0]),
                pltpu.make_async_copy(vc_hbm.at[layer], vbuf, kv_sem.at[1]))

    barrier = pltpu.get_barrier_semaphore()
    for other in (partner, peer):
        pl.semaphore_signal(barrier, inc=1, device_id={"model": other}, device_id_type=MESH)

    small = [pltpu.make_async_copy(src, dst, small_sem.at[k]) for k, (src, dst) in enumerate((
        (pos_hbm, pos_ref), (na_hbm, na_ref), (nm_hbm, nm_ref), (freq_hbm, freq_ref)))]

    def load_x(b, carry):
        pltpu.make_async_copy(x_hbm.at[:, pl.ds(pl.multiple_of(b * 128, 128), 128)], x.at[b], x_sem).start()
        return carry


    issue_qkv(0, 0)
    for cp in small:
        cp.start()
    lax.fori_loop(0, BLKS, load_x, 0)
    issue_qkv(0, 1)
    for cp in kv_copies(0):
        cp.start()
    issue_out(0, 0)
    issue_out(0, 1)
    for k in range(6):
        issue_gu(0, k // 2, k % 2)

    for cp in small:
        cp.wait()
    for layer in range(LAYERS):
        for which, ref in enumerate((na_ref, nm_ref)):
            row = ref[layer:layer + 1, :].astype(F32) * DOWN
            for blk in range(BLKS):
                gn[2 * layer + which, blk // 4, blk % 4:blk % 4 + 1, :] = row[:, blk * 128:(blk + 1) * 128]
    pos_row = jnp.broadcast_to(pos_ref[...].astype(F32), (ROWS, ROWS))
    ri = lax.broadcasted_iota(jnp.int32, (ROWS, ROWS), 0)
    ci = lax.broadcasted_iota(jnp.int32, (ROWS, ROWS), 1)
    pos_col = jnp.sum(jnp.where(ri == ci, pos_row, 0.0), axis=1, keepdims=True)
    pos_b = jnp.broadcast_to(pos_col, (ROWS, HD))
    posb[...] = pos_b
    angle = pos_b * freq_ref[...]
    cos_t[...] = jnp.cos(angle)
    sin_v = jnp.sin(angle)
    sin_t[...] = jnp.where(ci < HD // 2, -sin_v, sin_v)
    r2 = lax.broadcasted_iota(jnp.int32, (ROWS, GROUP * CACHE), 0)
    c2 = lax.broadcasted_iota(jnp.int32, (ROWS, GROUP * CACHE), 1)
    mine = (c2 // CACHE) == lax.rem(r2, GROUP)
    seen = lax.rem(c2, CACHE).astype(F32) <= jnp.broadcast_to(pos_col, (ROWS, GROUP * CACHE))
    vis[...] = jnp.where(mine & seen, 1.0, 0.0)
    cs = lax.broadcasted_iota(jnp.int32, (ROWS, CACHE), 1).astype(F32)
    mask16[...] = jnp.where(cs == jnp.broadcast_to(pos_col, (ROWS, CACHE)), 1.0, 0.0)

    pltpu.make_async_copy(x, x, x_sem).wait()
    pl.semaphore_wait(barrier, 2)

    def a_copy(j):
        return pltpu.make_async_remote_copy(a_send.at[j], a_recv.at[j], a_ss.at[j], a_rs.at[j],
                                            device_id={"model": partner}, device_id_type=MESH)

    def b_copy(p, j):
        return pltpu.make_async_remote_copy(b_send.at[j], b_recv.at[p, j], b_ss.at[j], b_rs.at[p, j],
                                            device_id={"model": peer}, device_id_type=MESH)

    def c_copy(j, half):
        blk = pl.ds(4 * j + 2 * half, 2)
        return pltpu.make_async_remote_copy(x.at[blk], x.at[blk], c_ss.at[j], c_rs.at[j],
                                            device_id={"model": partner}, device_id_type=MESH)

    def stage_a(j, part):
        first = core == 0
        for t in range(2):
            lo, hi = part[:, t * 128:(t + 1) * 128], part[:, (t + 2) * 128:(t + 3) * 128]
            own[j, t] = jnp.where(first, lo, hi)
            a_send[j, t] = jnp.where(first, hi, lo).astype(BF16)
        a_copy(j).start()

    def stage_b(p, j):
        a_copy(j).wait_recv()
        b_send[j] = (own[j] + a_recv[j].astype(F32)).astype(BF16)
        b_copy(p, j).start()

    def stage_c(p, j):
        b_copy(p, j).wait_recv()
        total = b_send[j].astype(F32) + b_recv[p, j].astype(F32)
        blk = pl.ds(4 * j + 2 * core, 2)
        x[blk] = (x[blk].astype(F32) + total).astype(BF16)
        c_copy(j, core).start()
        a_copy(j).wait_send()
        b_copy(p, j).wait_send()

    def stage_d(j):
        c_copy(j, 1 - core).wait_recv()
        c_copy(j, core).wait_send()

    def take(row, i):
        outs = []
        sq = ss[...]
        gains = gn[row, i]
        for b in range(4):
            blk = x[4 * i + b].astype(F32)
            sq = sq + blk * blk
            outs.append((blk * gains[b:b + 1, :]).astype(BF16))
        ss[...] = sq
        return jnp.concatenate(outs, axis=1)

    def row_scale():
        mean = jnp.sum(ss[...], axis=1, keepdims=True) * (1.0 / DIM)
        return lax.rsqrt(mean + NORM_EPS) * UP

    def dot(a, b):
        return jnp.dot(a, b, preferred_element_type=F32)

    def tiles(width, step):
        return [(n, min(step, width - n)) for n in range(0, width, step)]

    def layer_body(layer, carry):
        base = layer * PER_LAYER
        ss[...] = jnp.zeros_like(ss)
        qkv[...] = jnp.zeros((ROWS, QKV), F32)

        @pl.when(layer > 0)
        def _():
            stage_c(1, 0)

        def qkv_step(i, carry):
            @pl.when((layer > 0) & (i + 1 < PAIRS))
            def _():
                stage_c(1, i + 1)

            @pl.when(layer > 0)
            def _():
                stage_d(i)

            h = take(2 * layer, i)
            s = slot_of(base + i // 4)
            first = lax.rem(i, 4) * QKV
            for c0, w in tiles(QKV, 512):
                qkv[:, c0:c0 + w] += dot(h, ring[s, :, pl.ds(pl.multiple_of(first + c0, 128), w)])
            return carry

        wait_slot(base, 512, 4 * QKV)
        lax.fori_loop(0, 4, qkv_step, 0)
        issue_gu(layer, 3, 0)
        wait_slot(base + 1, 512, 3 * QKV)
        lax.fori_loop(4, PAIRS, qkv_step, 0)
        issue_gu(layer, 3, 1)

        scale = row_scale()
        cos_v, sin_v = cos_t[...], sin_t[...]

        def head(idx):
            return (qkv[:, idx * HD:(idx + 1) * HD] * scale).astype(BF16)

        def rotate(v):
            v = v.astype(F32)
            return (v * cos_v + pltpu.roll(v, HD // 2, axis=1) * sin_v).astype(BF16)

        for h in range(QH):
            qs[h][...] = rotate(head(h)).astype(F32)
        k_new = rotate(head(QH))
        v_new = head(QH + 1)
        kn[...] = k_new.astype(F32)
        vn[...] = v_new.astype(F32)
        rows_out = (pltpu.make_async_copy(kn16, kn_out.at[layer], row_sem.at[0]),
                    pltpu.make_async_copy(vn16, vn_out.at[layer], row_sem.at[1]))
        kn16[...] = k_new
        vn16[...] = v_new
        for cp in kv_copies(layer):
            cp.wait()
        wait_slot(base + 2, 512, DIM)
        wait_slot(base + 3, 384, DIM)
        srow = lax.rem(lax.broadcasted_iota(jnp.int32, (GROUP * CACHE, HD), 0), CACHE).astype(F32)

        def spread(v):
            return jnp.broadcast_to(v[:, None, :], (GROUP, CACHE, HD)).reshape(GROUP * CACHE, HD)

        span = [slice(g * GROUP, (g + 1) * GROUP) for g in range(GROUPS)]
        cspan = [slice(g * KEYS, (g + 1) * KEYS) for g in range(GROUPS)]
        for g in range(GROUPS):
            here = srow == spread(posb[span[g], :])
            kbuf[cspan[g], :] = jnp.where(here, spread(kn[span[g], :]), kbuf[cspan[g], :].astype(F32)).astype(BF16)
            vbuf[cspan[g], :] = jnp.where(here, spread(vn[span[g], :]), vbuf[cspan[g], :].astype(F32)).astype(BF16)
        for g in range(GROUPS):
            q = jnp.concatenate([qs[h][span[g], :] for h in range(QH)] + [qs[0][span[g], :]], axis=0).astype(BF16)
            sc[g][...] = lax.dot_general(q, kbuf[cspan[g], :], (((1,), (1,)), ((), ())), preferred_element_type=F32)
        for g in range(GROUPS):
            raw = (sc[g][...] * (HD ** -0.5)).reshape(QH + 1, GROUP, KEYS)
            raw = jnp.where((vis[span[g], :] > 0.5)[None], raw, -1e30)
            e = jnp.exp(raw - jnp.max(raw, axis=-1, keepdims=True))
            prob = e * (1.0 / jnp.sum(e, axis=-1, keepdims=True))
            pr[g][...] = prob.reshape(QROWS, KEYS).astype(BF16)
        for g in range(GROUPS):
            o = dot(pr[g][...], vbuf[cspan[g], :])
            for h in range(QH):
                at[h][span[g], :] = o[h * GROUP:(h + 1) * GROUP]

        for cp in rows_out:
            cp.start()

        @pl.when(layer + 1 < LAYERS)
        def _():
            for cp in kv_copies(layer + 1):
                cp.start()

        for h in range(QH):
            ab[:, h * HD:(h + 1) * HD] = at[h][...].astype(BF16)

        for j in range(PAIRS):
            cols = slice(j * 512, (j + 1) * 512)
            part = dot(ab[:, :512], ring[slot_of(base + 2), :, cols]) + dot(ab[:, 512:], ring[slot_of(base + 3), :384, cols])
            stage_a(j, part)
            if j >= 3:
                stage_b(0, j - 3)
        issue_gu(layer, 4, 0)
        issue_gu(layer, 4, 1)
        for j in range(PAIRS - 3, PAIRS):
            stage_b(0, j)

        ss[...] = jnp.zeros_like(ss)
        stage_c(0, 0)

        def gu_step(i, issue, first=False, last=False):
            if not last:
                stage_c(0, i + 1)
            stage_d(i)
            h = take(2 * layer + 1, i)
            n = base + 4 + 2 * i
            wait_slot(n, 512, FF)
            wait_slot(n + 1, 512, FF)
            for k, acc in ((0, acc_g), (1, acc_u)):
                s = slot_of(n + k)
                for c0, w in tiles(FF, 512):
                    part = dot(h, ring[s, :, c0:c0 + w])
                    if first:
                        acc[:, c0:c0 + w] = part
                    else:
                        acc[:, c0:c0 + w] += part
            issue(0)
            issue(1)

        gu_step(0, lambda k: issue_gu(layer, 5, k), first=True)
        gu_step(1, lambda k: issue_gu(layer, 6, k))

        def gu_mid(i, carry):
            gu_step(i, lambda k: issue_down(layer, 2 * (i - 2) + k))
            return carry

        lax.fori_loop(2, 5, gu_mid, 0)

        def more(fn):
            pl.when(layer + 1 < LAYERS)(fn)

        gu_step(5, lambda k: more(lambda: issue_qkv(layer + 1, 0)) if k else issue_down(layer, 6))
        gu_step(6, lambda k: more(lambda: issue_out(layer + 1, 0)) if k else more(lambda: issue_qkv(layer + 1, 1)), last=True)
        wait_slot(base + 18, 512, FF)
        scale2 = row_scale()
        for c0, w in tiles(FF, 512):
            gate = acc_g[:, c0:c0 + w] * scale2
            up = acc_u[:, c0:c0 + w] * scale2
            act[:, c0:c0 + w] = (gate * jax.nn.sigmoid(gate) * up).astype(BF16)

        def down_step(j, issue, lead):
            n = base + 18 + j
            s = slot_of(n)
            if lead:
                wait_slot(n, 512, FF)
            part = dot(act[:, :512], ring[s, :, :512])
            for b in range(1, 9):
                part = part + dot(act[:, b * 512:(b + 1) * 512], ring[s, :, b * 512:(b + 1) * 512])
            last = jnp.concatenate([ring[s, q * 128:(q + 1) * 128, 4608:4736] for q in range(4)], axis=1)
            part = part + dot(act[:, 4608:4736], last)
            stage_a(j, part)

            @pl.when(layer + 1 < LAYERS)
            def _():
                issue()

            if lead:
                stage_b(1, j - 1)

        down_step(0, lambda: issue_out(layer + 1, 1), False)

        def down_pair(t, carry):
            down_step(1 + 2 * t, lambda: issue_gu(layer + 1, t, 0), True)
            down_step(2 + 2 * t, lambda: issue_gu(layer + 1, t, 1), True)
            return carry

        lax.fori_loop(0, 3, down_pair, 0)
        stage_b(1, PAIRS - 1)
        for cp in rows_out:
            cp.wait()
        return carry

    mask_copy = pltpu.make_async_copy(mask16, mask_out, row_sem.at[2])
    mask_copy.start()
    lax.fori_loop(0, LAYERS, layer_body, 0)
    mask_copy.wait()

    stage_c(1, 0)

    def last_step(i, carry):
        @pl.when(i + 1 < PAIRS)
        def _():
            stage_c(1, i + 1)

        stage_d(i)
        for b in range(4):
            blk = 4 * i + b
            pltpu.make_async_copy(x.at[blk], out_hbm.at[:, pl.ds(pl.multiple_of(blk * 128, 128), 128)], x_sem).start()
        return carry

    lax.fori_loop(0, PAIRS, last_step, 0)
    pltpu.make_async_copy(x, x, x_sem).wait()


def fused_layers(x, positions, norm_attn, norm_mlp, wq, wk, wv, wo, wg, wu, wd, kc, vc):
    half = HD // 2
    freq = (np.float32(ROPE_BASE) ** (-np.arange(half, dtype=np.float32) / np.float32(half))).astype(np.float32)
    freq = jnp.asarray(np.concatenate([freq, freq])[None, :])
    hbm = pl.BlockSpec(memory_space=pl.ANY)
    vmem = pltpu.VMEM
    dma = pltpu.SemaphoreType.DMA
    scratch = [
        vmem((1, ROWS), jnp.int32), vmem((LAYERS, DIM), BF16), vmem((LAYERS, DIM), BF16), vmem((1, HD), F32), dma((4,)),
        vmem((ROWS, HD), BF16), vmem((ROWS, HD), BF16), vmem((ROWS, CACHE), F32), dma((3,)),
        vmem((SLOTS, 512, FF), BF16), dma((SLOTS,)),
        vmem((BLKS, ROWS, 128), BF16), dma,
        vmem((2 * LAYERS, PAIRS, 8, 128), F32),
        vmem((ROWS, HD), F32), vmem((ROWS, HD), F32), vmem((ROWS, HD), F32),
        vmem((ROWS, GROUP * CACHE), F32),
        vmem((ROWS, HD), F32),
        vmem((ROWS, HD), F32), vmem((ROWS, HD), F32), vmem((ROWS, QH * HD), BF16),
        vmem((ROWS, FF), F32), vmem((ROWS, FF), F32), vmem((ROWS, FF), BF16),
        vmem((ROWS * CACHE, HD), BF16), vmem((ROWS * CACHE, HD), BF16), dma((2,)),
        vmem((PAIRS, 2, ROWS, 128), F32),
        vmem((PAIRS, 2, ROWS, 128), BF16), vmem((PAIRS, 2, ROWS, 128), BF16),
        vmem((PAIRS, 2, ROWS, 128), BF16), vmem((2, PAIRS, 2, ROWS, 128), BF16),
        dma((PAIRS,)), dma((PAIRS,)), dma((PAIRS,)), dma((2, PAIRS)), dma((PAIRS,)), dma((PAIRS,)),
    ]
    new_rows = jax.ShapeDtypeStruct((LAYERS, ROWS, HD), BF16)
    return pl.pallas_call(
        kernel,
        out_shape=(jax.ShapeDtypeStruct((ROWS, DIM), BF16), new_rows, new_rows, jax.ShapeDtypeStruct((ROWS, CACHE), F32)),
        in_specs=[hbm] * 14,
        out_specs=(hbm,) * 4,
        scratch_shapes=scratch,
        compiler_params=pltpu.CompilerParams(collective_id=0, has_side_effects=True, vmem_limit_bytes=67043328),
        name="layers",
    )(x, positions, norm_attn, norm_mlp, freq, wq, wk, wv, wo, wg, wu, wd, kc, vc)


def solution(mesh):
    def local_step(hidden_in, positions, norm_attn, norm_mlp, w_query, w_key, w_value, w_out, w_gate, w_up, w_down, key_cache, value_cache):
        flat = (LAYERS, ROWS * CACHE, HD)
        hidden, k_new, v_new, mask = fused_layers(
            hidden_in, positions[None, :], norm_attn, norm_mlp, w_query, w_key, w_value, w_out, w_gate, w_up, w_down,
            key_cache.reshape(flat), value_cache.reshape(flat))
        write_row = (mask > 0.5)[None, :, :, None, None]
        key_out = jnp.where(write_row, k_new[:, :, None, None, :], key_cache)
        value_out = jnp.where(write_row, v_new[:, :, None, None, :], value_cache)
        return hidden, key_out, value_out

    row_spec = P("data", None)
    col_spec = P(None, None, "model")
    split_spec = P(None, "model", None)
    cache_spec = P(None, "data", None, "model", None)
    in_specs = (row_spec, P("data"), P(None, None), P(None, None), col_spec, col_spec, col_spec, split_spec, col_spec, col_spec, split_spec, cache_spec, cache_spec)
    out_specs = (row_spec, cache_spec, cache_spec)
    return jax.shard_map(local_step, mesh=mesh, in_specs=in_specs, out_specs=out_specs, check_vma=False)
```

```python
import functools

import jax
import jax.numpy as jnp
import numpy as np
from jax import lax
from jax.experimental import pallas as pl
from jax.experimental.pallas import tpu as pltpu
from jax.sharding import PartitionSpec as P

NORM_EPS = 1e-6
ROPE_BASE = 10000.0
MESH = pl.DeviceIdType.MESH
F32 = jnp.float32
BF16 = jnp.bfloat16

LAYERS = 3
ROWS = 128
DIM = 3584
HD = 128
QH = 7
CACHE = 32
FF = 4736
BLKS = DIM // 128
PAIRS = DIM // 512
QKV = (QH + 2) * HD
PER_LAYER = 2 + 2 + 2 * PAIRS + PAIRS
SLOTS = 10
DOWN = 2.0 ** -32
UP = 2.0 ** 32
GROUP = 8
GROUPS = ROWS // GROUP
QROWS = (QH + 1) * GROUP
KEYS = GROUP * CACHE


def kernel(x_hbm, pos_hbm, na_hbm, nm_hbm, freq_hbm, wq, wk, wv, wo, wg, wu, wd, kc_hbm, vc_hbm,
           out, kc_out, vc_out,
           pos_ref, na_ref, nm_ref, freq_ref, small_sem,
           ring, ring_sem, x, x_sem, gn, posb, cos_t, sin_t, vis, ss, kn, vn, ab, acc_g, acc_u, act,
           kv_sem, send, a_recv, b_recv, a_ss, a_rs, b_ss, b_rs, c_ss, c_rs):
    me = lax.axis_index("model")
    core = lax.rem(me, 2)
    partner = me + 1 - 2 * core
    peer = lax.rem(me + 2, 4)

    at = [acc_u.at[:, h * HD:(h + 1) * HD] for h in range(QH)]
    qs = [acc_u.at[:, (QH + h) * HD:(QH + h + 1) * HD] for h in range(QH)]
    qkv = acc_u.at[:, 2 * QH * HD:2 * QH * HD + QKV]
    sc = [acc_g.at[:QROWS, g * KEYS:(g + 1) * KEYS] for g in range(GROUPS)]
    pr = [act.at[:QROWS, g * KEYS:(g + 1) * KEYS] for g in range(GROUPS)]

    def slot_of(n):
        return lax.rem(n, SLOTS)

    def start(layer, r, src, rows, cols):
        s = slot_of(layer * PER_LAYER + r)
        pltpu.make_async_copy(src, ring.at[s, rows, cols], ring_sem.at[s]).start(priority=1)

    def issue_qkv(layer, r):
        for t in range(4 if r == 0 else 3):
            rows = slice((4 * r + t) * 512, (4 * r + t + 1) * 512)
            base = t * QKV
            start(layer, r, wq.at[layer, rows, :], slice(None), slice(base, base + QH * HD))
            start(layer, r, wk.at[layer, rows, :], slice(None), slice(base + QH * HD, base + (QH + 1) * HD))
            start(layer, r, wv.at[layer, rows, :], slice(None), slice(base + (QH + 1) * HD, base + QKV))

    def issue_out(layer, r):
        if r == 0:
            start(layer, 2, wo.at[layer, 0:512, :], slice(None), slice(0, DIM))
        else:
            start(layer, 3, wo.at[layer, 512:896, :], slice(0, 384), slice(0, DIM))

    def issue_gu(layer, i, which):
        rows = pl.ds(i * 512 if isinstance(i, int) else pl.multiple_of(i * 512, 512), 512)
        src = wu if which else wg
        start(layer, 4 + 2 * i + which, src.at[layer, rows, :], slice(None), slice(None))

    def issue_down(layer, j):
        off = j * 512 if isinstance(j, int) else pl.multiple_of(j * 512, 512)
        for b in range(9):
            start(layer, 18 + j, wd.at[layer, b * 512:(b + 1) * 512, pl.ds(off, 512)], slice(None), slice(b * 512, (b + 1) * 512))
        for q in range(4):
            cols = pl.ds(off + q * 128 if isinstance(j, int) else pl.multiple_of(off + q * 128, 128), 128)
            start(layer, 18 + j, wd.at[layer, 4608:4736, cols], slice(q * 128, (q + 1) * 128), slice(4608, 4736))

    def wait_slot(n, rows, cols):
        s = slot_of(n)
        pltpu.make_async_copy(wg.at[0, :rows, :cols], ring.at[s, :rows, :cols], ring_sem.at[s]).wait()

    def kv_copies(layer):
        return (pltpu.make_async_copy(kc_hbm.at[layer], kc_out.at[layer], kv_sem.at[0]),
                pltpu.make_async_copy(vc_hbm.at[layer], vc_out.at[layer], kv_sem.at[1]))

    barrier = pltpu.get_barrier_semaphore()
    for other in (partner, peer):
        pl.semaphore_signal(barrier, inc=1, device_id={"model": other}, device_id_type=MESH)

    small = [pltpu.make_async_copy(src, dst, small_sem.at[k]) for k, (src, dst) in enumerate((
        (pos_hbm, pos_ref), (na_hbm, na_ref), (nm_hbm, nm_ref), (freq_hbm, freq_ref)))]

    def load_x(b, carry):
        pltpu.make_async_copy(x_hbm.at[:, pl.ds(pl.multiple_of(b * 128, 128), 128)], x.at[b], x_sem).start()
        return carry


    issue_qkv(0, 0)
    for cp in small:
        cp.start()
    lax.fori_loop(0, BLKS, load_x, 0)
    issue_qkv(0, 1)
    for cp in kv_copies(0):
        cp.start()
    issue_out(0, 0)
    issue_out(0, 1)
    for k in range(6):
        issue_gu(0, k // 2, k % 2)

    for cp in small:
        cp.wait()
    for layer in range(LAYERS):
        for which, ref in enumerate((na_ref, nm_ref)):
            row = ref[layer:layer + 1, :].astype(F32) * DOWN
            for blk in range(BLKS):
                gn[2 * layer + which, blk // 4, blk % 4:blk % 4 + 1, :] = row[:, blk * 128:(blk + 1) * 128]
    pos_row = jnp.broadcast_to(pos_ref[...].astype(F32), (ROWS, ROWS))
    ri = lax.broadcasted_iota(jnp.int32, (ROWS, ROWS), 0)
    ci = lax.broadcasted_iota(jnp.int32, (ROWS, ROWS), 1)
    pos_col = jnp.sum(jnp.where(ri == ci, pos_row, 0.0), axis=1, keepdims=True)
    pos_b = jnp.broadcast_to(pos_col, (ROWS, HD))
    posb[...] = pos_b
    angle = pos_b * freq_ref[...]
    cos_t[...] = jnp.cos(angle)
    sin_v = jnp.sin(angle)
    sin_t[...] = jnp.where(ci < HD // 2, -sin_v, sin_v)
    r2 = lax.broadcasted_iota(jnp.int32, (ROWS, GROUP * CACHE), 0)
    c2 = lax.broadcasted_iota(jnp.int32, (ROWS, GROUP * CACHE), 1)
    mine = (c2 // CACHE) == lax.rem(r2, GROUP)
    seen = lax.rem(c2, CACHE).astype(F32) <= jnp.broadcast_to(pos_col, (ROWS, GROUP * CACHE))
    vis[...] = jnp.where(mine & seen, 1.0, 0.0)

    pltpu.make_async_copy(x, x, x_sem).wait()
    pl.semaphore_wait(barrier, 2)

    def a_copy(j):
        return pltpu.make_async_remote_copy(send.at[j], a_recv.at[j], a_ss.at[j], a_rs.at[j],
                                            device_id={"model": partner}, device_id_type=MESH)

    def b_copy(p, j):
        return pltpu.make_async_remote_copy(send.at[j], b_recv.at[p, j], b_ss.at[j], b_rs.at[p, j],
                                            device_id={"model": peer}, device_id_type=MESH)

    def c_copy(j, half):
        blk = pl.ds(4 * j + 2 * half, 2)
        return pltpu.make_async_remote_copy(x.at[blk], x.at[blk], c_ss.at[j], c_rs.at[j],
                                            device_id={"model": partner}, device_id_type=MESH)

    def own_cols(j, t):
        off = 2 * QH * HD + QKV + (2 * j + t) * 128
        return pl.ds(off if isinstance(j, int) else pl.multiple_of(off, 128), 128)

    def stage_a(j, part):
        first = core == 0
        for t in range(2):
            lo, hi = part[:, t * 128:(t + 1) * 128], part[:, (t + 2) * 128:(t + 3) * 128]
            acc_u[:, own_cols(j, t)] = jnp.where(first, lo, hi)
            send[j, t] = jnp.where(first, hi, lo).astype(BF16)
        a_copy(j).start()

    def stage_b(p, j):
        a_copy(j).wait_recv()
        a_copy(j).wait_send()
        for t in range(2):
            send[j, t] = (acc_u[:, own_cols(j, t)] + a_recv[j, t].astype(F32)).astype(BF16)
        b_copy(p, j).start()

    def stage_c(p, j):
        b_copy(p, j).wait_recv()
        total = send[j].astype(F32) + b_recv[p, j].astype(F32)
        blk = pl.ds(4 * j + 2 * core, 2)
        x[blk] = (x[blk].astype(F32) + total).astype(BF16)
        c_copy(j, core).start()
        b_copy(p, j).wait_send()

    def stage_d(j):
        c_copy(j, 1 - core).wait_recv()
        c_copy(j, core).wait_send()

    def take(row, i):
        outs = []
        sq = ss[...]
        gains = gn[row, i]
        for b in range(4):
            blk = x[4 * i + b].astype(F32)
            sq = sq + blk * blk
            outs.append((blk * gains[b:b + 1, :]).astype(BF16))
        ss[...] = sq
        return jnp.concatenate(outs, axis=1)

    def row_scale():
        mean = jnp.sum(ss[...], axis=1, keepdims=True) * (1.0 / DIM)
        return lax.rsqrt(mean + NORM_EPS) * UP

    def dot(a, b):
        return jnp.dot(a, b, preferred_element_type=F32)

    def tiles(width, step):
        return [(n, min(step, width - n)) for n in range(0, width, step)]

    def layer_body(layer, carry):
        base = layer * PER_LAYER
        ss[...] = jnp.zeros_like(ss)
        qkv[...] = jnp.zeros((ROWS, QKV), F32)

        @pl.when(layer > 0)
        def _():
            stage_c(1, 0)

        def qkv_step(i, carry):
            @pl.when((layer > 0) & (i + 1 < PAIRS))
            def _():
                stage_c(1, i + 1)

            @pl.when(layer > 0)
            def _():
                stage_d(i)

            h = take(2 * layer, i)
            s = slot_of(base + i // 4)
            first = lax.rem(i, 4) * QKV
            for c0, w in tiles(QKV, 512):
                qkv[:, c0:c0 + w] += dot(h, ring[s, :, pl.ds(pl.multiple_of(first + c0, 128), w)])
            return carry

        wait_slot(base, 512, 4 * QKV)
        lax.fori_loop(0, 4, qkv_step, 0)
        issue_gu(layer, 3, 0)
        wait_slot(base + 1, 512, 3 * QKV)
        lax.fori_loop(4, PAIRS, qkv_step, 0)
        issue_gu(layer, 3, 1)

        scale = row_scale()
        cos_v, sin_v = cos_t[...], sin_t[...]

        def head(idx):
            return (qkv[:, idx * HD:(idx + 1) * HD] * scale).astype(BF16)

        def rotate(v):
            v = v.astype(F32)
            return (v * cos_v + pltpu.roll(v, HD // 2, axis=1) * sin_v).astype(BF16)

        for h in range(QH):
            qs[h][...] = rotate(head(h)).astype(F32)
        k_new = rotate(head(QH))
        v_new = head(QH + 1)
        kn[...] = k_new.astype(F32)
        vn[...] = v_new.astype(F32)
        for cp in kv_copies(layer):
            cp.wait()
        wait_slot(base + 2, 512, DIM)
        wait_slot(base + 3, 384, DIM)
        srow = lax.rem(lax.broadcasted_iota(jnp.int32, (GROUP * CACHE, HD), 0), CACHE).astype(F32)

        def spread(v):
            return jnp.broadcast_to(v[:, None, :], (GROUP, CACHE, HD)).reshape(GROUP * CACHE, HD)

        span = [slice(g * GROUP, (g + 1) * GROUP) for g in range(GROUPS)]
        cspan = [slice(g * KEYS, (g + 1) * KEYS) for g in range(GROUPS)]
        for g in range(GROUPS):
            here = srow == spread(posb[span[g], :])
            kc_out[layer, cspan[g], :] = jnp.where(here, spread(kn[span[g], :]), kc_out[layer, cspan[g], :].astype(F32)).astype(BF16)
            vc_out[layer, cspan[g], :] = jnp.where(here, spread(vn[span[g], :]), vc_out[layer, cspan[g], :].astype(F32)).astype(BF16)
        for g in range(GROUPS):
            q = jnp.concatenate([qs[h][span[g], :] for h in range(QH)] + [qs[0][span[g], :]], axis=0).astype(BF16)
            sc[g][...] = lax.dot_general(q, kc_out[layer, cspan[g], :], (((1,), (1,)), ((), ())), preferred_element_type=F32)
        for g in range(GROUPS):
            raw = (sc[g][...] * (HD ** -0.5)).reshape(QH + 1, GROUP, KEYS)
            raw = jnp.where((vis[span[g], :] > 0.5)[None], raw, -1e30)
            e = jnp.exp(raw - jnp.max(raw, axis=-1, keepdims=True))
            prob = e * (1.0 / jnp.sum(e, axis=-1, keepdims=True))
            pr[g][...] = prob.reshape(QROWS, KEYS).astype(BF16)
        for g in range(GROUPS):
            o = dot(pr[g][...], vc_out[layer, cspan[g], :])
            for h in range(QH):
                at[h][span[g], :] = o[h * GROUP:(h + 1) * GROUP]

        @pl.when(layer + 1 < LAYERS)
        def _():
            for cp in kv_copies(layer + 1):
                cp.start()

        for h in range(QH):
            ab[:, h * HD:(h + 1) * HD] = at[h][...].astype(BF16)

        for j in range(PAIRS):
            cols = slice(j * 512, (j + 1) * 512)
            part = dot(ab[:, :512], ring[slot_of(base + 2), :, cols]) + dot(ab[:, 512:], ring[slot_of(base + 3), :384, cols])
            stage_a(j, part)
            if j >= 3:
                stage_b(0, j - 3)
        issue_gu(layer, 4, 0)
        issue_gu(layer, 4, 1)
        for j in range(PAIRS - 3, PAIRS):
            stage_b(0, j)

        ss[...] = jnp.zeros_like(ss)
        stage_c(0, 0)

        def gu_step(i, issue, first=False, last=False):
            if not last:
                stage_c(0, i + 1)
            stage_d(i)
            h = take(2 * layer + 1, i)
            n = base + 4 + 2 * i
            wait_slot(n, 512, FF)
            wait_slot(n + 1, 512, FF)
            for k, acc in ((0, acc_g), (1, acc_u)):
                s = slot_of(n + k)
                for c0, w in tiles(FF, 512):
                    part = dot(h, ring[s, :, c0:c0 + w])
                    if first:
                        acc[:, c0:c0 + w] = part
                    else:
                        acc[:, c0:c0 + w] += part
            issue(0)
            issue(1)

        gu_step(0, lambda k: issue_gu(layer, 5, k), first=True)
        gu_step(1, lambda k: issue_gu(layer, 6, k))

        def gu_mid(i, carry):
            gu_step(i, lambda k: issue_down(layer, 2 * (i - 2) + k))
            return carry

        lax.fori_loop(2, 5, gu_mid, 0)

        def more(fn):
            pl.when(layer + 1 < LAYERS)(fn)

        gu_step(5, lambda k: more(lambda: issue_qkv(layer + 1, 0)) if k else issue_down(layer, 6))
        gu_step(6, lambda k: more(lambda: issue_out(layer + 1, 0)) if k else more(lambda: issue_qkv(layer + 1, 1)), last=True)
        wait_slot(base + 18, 512, FF)
        scale2 = row_scale()
        for c0, w in tiles(FF, 512):
            gate = acc_g[:, c0:c0 + w] * scale2
            up = acc_u[:, c0:c0 + w] * scale2
            act[:, c0:c0 + w] = (gate * jax.nn.sigmoid(gate) * up).astype(BF16)

        def down_step(j, issue, lead):
            n = base + 18 + j
            s = slot_of(n)
            if lead:
                wait_slot(n, 512, FF)
            part = dot(act[:, :512], ring[s, :, :512])
            for b in range(1, 9):
                part = part + dot(act[:, b * 512:(b + 1) * 512], ring[s, :, b * 512:(b + 1) * 512])
            last = jnp.concatenate([ring[s, q * 128:(q + 1) * 128, 4608:4736] for q in range(4)], axis=1)
            part = part + dot(act[:, 4608:4736], last)
            stage_a(j, part)

            @pl.when(layer + 1 < LAYERS)
            def _():
                issue()

            if lead:
                stage_b(1, j - 1)

        down_step(0, lambda: issue_out(layer + 1, 1), False)

        def down_pair(t, carry):
            down_step(1 + 2 * t, lambda: issue_gu(layer + 1, t, 0), True)
            down_step(2 + 2 * t, lambda: issue_gu(layer + 1, t, 1), True)
            return carry

        lax.fori_loop(0, 3, down_pair, 0)
        stage_b(1, PAIRS - 1)
        return carry

    lax.fori_loop(0, LAYERS, layer_body, 0)

    stage_c(1, 0)

    def last_step(i, carry):
        @pl.when(i + 1 < PAIRS)
        def _():
            stage_c(1, i + 1)

        stage_d(i)
        for b in range(4):
            blk = 4 * i + b
            out[:, pl.ds(pl.multiple_of(blk * 128, 128), 128)] = x[blk]
        return carry

    lax.fori_loop(0, PAIRS, last_step, 0)


def fused_layers(x, positions, norm_attn, norm_mlp, wq, wk, wv, wo, wg, wu, wd, kc, vc):
    half = HD // 2
    freq = (np.float32(ROPE_BASE) ** (-np.arange(half, dtype=np.float32) / np.float32(half))).astype(np.float32)
    freq = jnp.asarray(np.concatenate([freq, freq])[None, :])
    hbm = pl.BlockSpec(memory_space=pl.ANY)
    vmem = pltpu.VMEM
    dma = pltpu.SemaphoreType.DMA
    scratch = [
        vmem((1, ROWS), jnp.int32), vmem((LAYERS, DIM), BF16), vmem((LAYERS, DIM), BF16), vmem((1, HD), F32), dma((4,)),
                vmem((SLOTS, 512, FF), BF16), dma((SLOTS,)),
        vmem((BLKS, ROWS, 128), BF16), dma,
        vmem((2 * LAYERS, PAIRS, 8, 128), F32),
        vmem((ROWS, HD), F32), vmem((ROWS, HD), F32), vmem((ROWS, HD), F32),
        vmem((ROWS, GROUP * CACHE), F32),
        vmem((ROWS, HD), F32),
        vmem((ROWS, HD), F32), vmem((ROWS, HD), F32), vmem((ROWS, QH * HD), BF16),
        vmem((ROWS, FF), F32), vmem((ROWS, FF), F32), vmem((ROWS, FF), BF16),
        dma((2,)),
        vmem((PAIRS, 2, ROWS, 128), BF16), vmem((PAIRS, 2, ROWS, 128), BF16),
        vmem((2, PAIRS, 2, ROWS, 128), BF16),
        dma((PAIRS,)), dma((PAIRS,)), dma((PAIRS,)), dma((2, PAIRS)), dma((PAIRS,)), dma((PAIRS,)),
    ]
    caches = vmem((LAYERS, ROWS * CACHE, HD), BF16)
    vm = pl.BlockSpec(memory_space=pltpu.VMEM)
    return pl.pallas_call(
        kernel,
        out_shape=(vmem((ROWS, DIM), BF16), caches, caches),
        in_specs=[hbm] * 14,
        out_specs=(vm, vm, vm),
        scratch_shapes=scratch,
        compiler_params=pltpu.CompilerParams(collective_id=0, has_side_effects=True, vmem_limit_bytes=59800000),
        name="layers",
    )(x, positions, norm_attn, norm_mlp, freq, wq, wk, wv, wo, wg, wu, wd, kc, vc)


def solution(mesh):
    def local_step(hidden_in, positions, norm_attn, norm_mlp, w_query, w_key, w_value, w_out, w_gate, w_up, w_down, key_cache, value_cache):
        flat = (LAYERS, ROWS * CACHE, HD)
        hidden, k_out, v_out = fused_layers(
            hidden_in, positions[None, :], norm_attn, norm_mlp, w_query, w_key, w_value, w_out, w_gate, w_up, w_down,
            key_cache.reshape(flat), value_cache.reshape(flat))
        return hidden, k_out.reshape(key_cache.shape), v_out.reshape(value_cache.shape)

    row_spec = P("data", None)
    col_spec = P(None, None, "model")
    split_spec = P(None, "model", None)
    cache_spec = P(None, "data", None, "model", None)
    in_specs = (row_spec, P("data"), P(None, None), P(None, None), col_spec, col_spec, col_spec, split_spec, col_spec, col_spec, split_spec, cache_spec, cache_spec)
    out_specs = (row_spec, cache_spec, cache_spec)
    return jax.shard_map(local_step, mesh=mesh, in_specs=in_specs, out_specs=out_specs, check_vma=False)
```

```python
import functools

import jax
import jax.numpy as jnp
import numpy as np
from jax import lax
from jax.experimental import pallas as pl
from jax.experimental.pallas import tpu as pltpu
from jax.sharding import PartitionSpec as P

NORM_EPS = 1e-6
ROPE_BASE = 10000.0
MESH = pl.DeviceIdType.MESH
F32 = jnp.float32
BF16 = jnp.bfloat16

LAYERS = 3
ROWS = 128
DIM = 3584
HD = 128
QH = 7
CACHE = 32
FF = 4736
BLKS = DIM // 128
PAIRS = DIM // 512
QKV = (QH + 2) * HD
PER_LAYER = 2 + 2 + 2 * PAIRS + PAIRS
SLOTS = 10
DOWN = 2.0 ** -32
UP = 2.0 ** 32
GROUP = 8
GROUPS = ROWS // GROUP
QROWS = (QH + 1) * GROUP
KEYS = GROUP * CACHE


def kernel(x_hbm, pos_hbm, na_hbm, nm_hbm, freq_hbm, wq, wk, wv, wo, wg, wu, wd, kc_hbm, vc_hbm,
           out, kc_out, vc_out,
           pos_ref, na_ref, nm_ref, freq_ref, small_sem,
           ring, ring_sem, x, x_sem, gn, posb, cos_t, sin_t, vis, ss, kn, vn, ab, acc_g, acc_u, act,
           kv_sem, send, a_recv, b_recv, a_ss, a_rs, b_ss, b_rs, c_ss, c_rs):
    me = lax.axis_index("model")
    core = lax.rem(me, 2)
    partner = me + 1 - 2 * core
    peer = lax.rem(me + 2, 4)

    at = [acc_u.at[:, h * HD:(h + 1) * HD] for h in range(QH)]
    qs = [acc_u.at[:, (QH + h) * HD:(QH + h + 1) * HD] for h in range(QH)]
    qkv = acc_u.at[:, 2 * QH * HD:2 * QH * HD + QKV]
    sc = [acc_g.at[:QROWS, g * KEYS:(g + 1) * KEYS] for g in range(GROUPS)]
    pr = [act.at[:QROWS, g * KEYS:(g + 1) * KEYS] for g in range(GROUPS)]

    def slot_of(n):
        return lax.rem(n, SLOTS)

    def start(layer, r, src, rows, cols):
        s = slot_of(layer * PER_LAYER + r)
        pltpu.make_async_copy(src, ring.at[s, rows, cols], ring_sem.at[s]).start(priority=1)

    def issue_qkv(layer, r):
        for t in range(4 if r == 0 else 3):
            rows = slice((4 * r + t) * 512, (4 * r + t + 1) * 512)
            base = t * QKV
            start(layer, r, wq.at[layer, rows, :], slice(None), slice(base, base + QH * HD))
            start(layer, r, wk.at[layer, rows, :], slice(None), slice(base + QH * HD, base + (QH + 1) * HD))
            start(layer, r, wv.at[layer, rows, :], slice(None), slice(base + (QH + 1) * HD, base + QKV))

    def issue_out(layer, r):
        if r == 0:
            start(layer, 2, wo.at[layer, 0:512, :], slice(None), slice(0, DIM))
        else:
            start(layer, 3, wo.at[layer, 512:896, :], slice(0, 384), slice(0, DIM))

    def issue_gu(layer, i, which):
        rows = pl.ds(i * 512 if isinstance(i, int) else pl.multiple_of(i * 512, 512), 512)
        src = wu if which else wg
        start(layer, 4 + 2 * i + which, src.at[layer, rows, :], slice(None), slice(None))

    def issue_down(layer, j):
        off = j * 512 if isinstance(j, int) else pl.multiple_of(j * 512, 512)
        for b in range(9):
            start(layer, 18 + j, wd.at[layer, b * 512:(b + 1) * 512, pl.ds(off, 512)], slice(None), slice(b * 512, (b + 1) * 512))
        for q in range(4):
            cols = pl.ds(off + q * 128 if isinstance(j, int) else pl.multiple_of(off + q * 128, 128), 128)
            start(layer, 18 + j, wd.at[layer, 4608:4736, cols], slice(q * 128, (q + 1) * 128), slice(4608, 4736))

    def wait_slot(n, rows, cols):
        s = slot_of(n)
        pltpu.make_async_copy(wg.at[0, :rows, :cols], ring.at[s, :rows, :cols], ring_sem.at[s]).wait()

    def kv_copies(layer):
        return (pltpu.make_async_copy(kc_hbm.at[layer], kc_out.at[layer], kv_sem.at[0]),
                pltpu.make_async_copy(vc_hbm.at[layer], vc_out.at[layer], kv_sem.at[1]))

    barrier = pltpu.get_barrier_semaphore()
    for other in (partner, peer):
        pl.semaphore_signal(barrier, inc=1, device_id={"model": other}, device_id_type=MESH)

    small = [pltpu.make_async_copy(src, dst, small_sem.at[k]) for k, (src, dst) in enumerate((
        (pos_hbm, pos_ref), (na_hbm, na_ref), (nm_hbm, nm_ref), (freq_hbm, freq_ref)))]

    def load_x(b, carry):
        pltpu.make_async_copy(x_hbm.at[:, pl.ds(pl.multiple_of(b * 128, 128), 128)], x.at[b], x_sem).start()
        return carry


    issue_qkv(0, 0)
    for cp in small:
        cp.start()
    lax.fori_loop(0, BLKS, load_x, 0)
    issue_qkv(0, 1)
    for cp in kv_copies(0):
        cp.start()
    issue_out(0, 0)
    issue_out(0, 1)
    for k in range(6):
        issue_gu(0, k // 2, k % 2)

    for cp in small:
        cp.wait()
    for layer in range(LAYERS):
        for which, ref in enumerate((na_ref, nm_ref)):
            row = ref[layer:layer + 1, :].astype(F32) * DOWN
            for blk in range(BLKS):
                gn[2 * layer + which, blk // 4, blk % 4:blk % 4 + 1, :] = row[:, blk * 128:(blk + 1) * 128]
    pos_row = jnp.broadcast_to(pos_ref[...].astype(F32), (ROWS, ROWS))
    ri = lax.broadcasted_iota(jnp.int32, (ROWS, ROWS), 0)
    ci = lax.broadcasted_iota(jnp.int32, (ROWS, ROWS), 1)
    pos_col = jnp.sum(jnp.where(ri == ci, pos_row, 0.0), axis=1, keepdims=True)
    pos_b = jnp.broadcast_to(pos_col, (ROWS, HD))
    posb[...] = pos_b
    angle = pos_b * freq_ref[...]
    cos_t[...] = jnp.cos(angle)
    sin_v = jnp.sin(angle)
    sin_t[...] = jnp.where(ci < HD // 2, -sin_v, sin_v)
    r2 = lax.broadcasted_iota(jnp.int32, (ROWS, GROUP * CACHE), 0)
    c2 = lax.broadcasted_iota(jnp.int32, (ROWS, GROUP * CACHE), 1)
    mine = (c2 // CACHE) == lax.rem(r2, GROUP)
    seen = lax.rem(c2, CACHE).astype(F32) <= jnp.broadcast_to(pos_col, (ROWS, GROUP * CACHE))
    vis[...] = jnp.where(mine & seen, 1.0, 0.0)

    pltpu.make_async_copy(x, x, x_sem).wait()
    pl.semaphore_wait(barrier, 2)

    def a_copy(j):
        return pltpu.make_async_remote_copy(send.at[j], a_recv.at[j], a_ss.at[j], a_rs.at[j],
                                            device_id={"model": partner}, device_id_type=MESH)

    def b_copy(p, j):
        return pltpu.make_async_remote_copy(send.at[j], b_recv.at[p, j], b_ss.at[j], b_rs.at[p, j],
                                            device_id={"model": peer}, device_id_type=MESH)

    def c_copy(j, half):
        blk = pl.ds(4 * j + 2 * half, 2)
        return pltpu.make_async_remote_copy(x.at[blk], x.at[blk], c_ss.at[j], c_rs.at[j],
                                            device_id={"model": partner}, device_id_type=MESH)

    def own_cols(j, t):
        off = 2 * QH * HD + QKV + (2 * j + t) * 128
        return pl.ds(off if isinstance(j, int) else pl.multiple_of(off, 128), 128)

    def stage_a(j, part):
        first = core == 0
        for t in range(2):
            lo, hi = part[:, t * 128:(t + 1) * 128], part[:, (t + 2) * 128:(t + 3) * 128]
            acc_u[:, own_cols(j, t)] = jnp.where(first, lo, hi)
            send[j, t] = jnp.where(first, hi, lo).astype(BF16)
        a_copy(j).start()

    def stage_b(p, j):
        a_copy(j).wait_recv()
        a_copy(j).wait_send()
        for t in range(2):
            send[j, t] = (acc_u[:, own_cols(j, t)] + a_recv[j, t].astype(F32)).astype(BF16)
        b_copy(p, j).start()

    def stage_c(p, j):
        b_copy(p, j).wait_recv()
        total = send[j].astype(F32) + b_recv[p, j].astype(F32)
        blk = pl.ds(4 * j + 2 * core, 2)
        x[blk] = (x[blk].astype(F32) + total).astype(BF16)
        c_copy(j, core).start()
        b_copy(p, j).wait_send()

    def stage_d(j):
        c_copy(j, 1 - core).wait_recv()
        c_copy(j, core).wait_send()

    def take(row, i):
        outs = []
        sq = ss[...]
        gains = gn[row, i]
        for b in range(4):
            blk = x[4 * i + b].astype(F32)
            sq = sq + blk * blk
            outs.append((blk * gains[b:b + 1, :]).astype(BF16))
        ss[...] = sq
        return jnp.concatenate(outs, axis=1)

    def row_scale():
        mean = jnp.sum(ss[...], axis=1, keepdims=True) * (1.0 / DIM)
        return lax.rsqrt(mean + NORM_EPS) * UP

    def dot(a, b):
        return jnp.dot(a, b, preferred_element_type=F32)

    def tiles(width, step):
        return [(n, min(step, width - n)) for n in range(0, width, step)]

    def layer_body(layer, carry):
        base = layer * PER_LAYER
        ss[...] = jnp.zeros_like(ss)
        qkv[...] = jnp.zeros((ROWS, QKV), F32)

        @pl.when(layer > 0)
        def _():
            stage_c(1, 0)

        def qkv_step(i, carry):
            @pl.when((layer > 0) & (i + 1 < PAIRS))
            def _():
                stage_c(1, i + 1)

            @pl.when(layer > 0)
            def _():
                stage_d(i)

            h = take(2 * layer, i)
            s = slot_of(base + i // 4)
            first = lax.rem(i, 4) * QKV
            for c0, w in tiles(QKV, 512):
                qkv[:, c0:c0 + w] += dot(h, ring[s, :, pl.ds(pl.multiple_of(first + c0, 128), w)])
            return carry

        wait_slot(base, 512, 4 * QKV)
        lax.fori_loop(0, 4, qkv_step, 0)
        issue_gu(layer, 3, 0)
        wait_slot(base + 1, 512, 3 * QKV)
        lax.fori_loop(4, PAIRS, qkv_step, 0)
        issue_gu(layer, 3, 1)

        scale = row_scale()
        cos_v, sin_v = cos_t[...], sin_t[...]

        def head(idx):
            return (qkv[:, idx * HD:(idx + 1) * HD] * scale).astype(BF16)

        def rotate(v):
            v = v.astype(F32)
            return (v * cos_v + pltpu.roll(v, HD // 2, axis=1) * sin_v).astype(BF16)

        for h in range(QH):
            qs[h][...] = rotate(head(h)).astype(F32)
        k_new = rotate(head(QH))
        v_new = head(QH + 1)
        kn[...] = k_new.astype(F32)
        vn[...] = v_new.astype(F32)
        for cp in kv_copies(layer):
            cp.wait()
        wait_slot(base + 2, 512, DIM)
        wait_slot(base + 3, 384, DIM)
        srow = lax.broadcasted_iota(jnp.int32, (CACHE, HD), 0).astype(F32).astype(BF16)

        def spread(v):
            return jnp.broadcast_to(v[:, None, :], (GROUP, CACHE, HD)).reshape(GROUP * CACHE, HD)

        span = [slice(g * GROUP, (g + 1) * GROUP) for g in range(GROUPS)]
        cspan = [slice(g * KEYS, (g + 1) * KEYS) for g in range(GROUPS)]
        for t in range(ROWS):
            trow = slice(t * CACHE, (t + 1) * CACHE)
            here = srow == jnp.broadcast_to(posb[t:t + 1, :], (CACHE, HD)).astype(BF16)
            k_row = jnp.broadcast_to(kn[t:t + 1, :], (CACHE, HD)).astype(BF16)
            v_row = jnp.broadcast_to(vn[t:t + 1, :], (CACHE, HD)).astype(BF16)
            kc_out[layer, trow, :] = jnp.where(here, k_row, kc_out[layer, trow, :])
            vc_out[layer, trow, :] = jnp.where(here, v_row, vc_out[layer, trow, :])
        for g in range(GROUPS):
            q = jnp.concatenate([qs[h][span[g], :] for h in range(QH)] + [qs[0][span[g], :]], axis=0).astype(BF16)
            sc[g][...] = lax.dot_general(q, kc_out[layer, cspan[g], :], (((1,), (1,)), ((), ())), preferred_element_type=F32)
        for g in range(GROUPS):
            raw = (sc[g][...] * (HD ** -0.5)).reshape(QH + 1, GROUP, KEYS)
            raw = jnp.where((vis[span[g], :] > 0.5)[None], raw, -1e30)
            e = jnp.exp(raw - jnp.max(raw, axis=-1, keepdims=True))
            prob = e * (1.0 / jnp.sum(e, axis=-1, keepdims=True))
            pr[g][...] = prob.reshape(QROWS, KEYS).astype(BF16)
        for g in range(GROUPS):
            o = dot(pr[g][...], vc_out[layer, cspan[g], :])
            for h in range(QH):
                at[h][span[g], :] = o[h * GROUP:(h + 1) * GROUP]

        @pl.when(layer + 1 < LAYERS)
        def _():
            for cp in kv_copies(layer + 1):
                cp.start()

        for h in range(QH):
            ab[:, h * HD:(h + 1) * HD] = at[h][...].astype(BF16)

        for j in range(PAIRS):
            cols = slice(j * 512, (j + 1) * 512)
            part = dot(ab[:, :512], ring[slot_of(base + 2), :, cols]) + dot(ab[:, 512:], ring[slot_of(base + 3), :384, cols])
            stage_a(j, part)
            if j >= 3:
                stage_b(0, j - 3)
        issue_gu(layer, 4, 0)
        issue_gu(layer, 4, 1)
        for j in range(PAIRS - 3, PAIRS):
            stage_b(0, j)

        ss[...] = jnp.zeros_like(ss)
        stage_c(0, 0)

        def gu_step(i, issue, first=False, last=False):
            if not last:
                stage_c(0, i + 1)
            stage_d(i)
            h = take(2 * layer + 1, i)
            n = base + 4 + 2 * i
            wait_slot(n, 512, FF)
            wait_slot(n + 1, 512, FF)
            for k, acc in ((0, acc_g), (1, acc_u)):
                s = slot_of(n + k)
                for c0, w in tiles(FF, 512):
                    part = dot(h, ring[s, :, c0:c0 + w])
                    if first:
                        acc[:, c0:c0 + w] = part
                    else:
                        acc[:, c0:c0 + w] += part
            issue(0)
            issue(1)

        gu_step(0, lambda k: issue_gu(layer, 5, k), first=True)
        gu_step(1, lambda k: issue_gu(layer, 6, k))

        def gu_mid(i, carry):
            gu_step(i, lambda k: issue_down(layer, 2 * (i - 2) + k))
            return carry

        lax.fori_loop(2, 5, gu_mid, 0)

        def more(fn):
            pl.when(layer + 1 < LAYERS)(fn)

        gu_step(5, lambda k: more(lambda: issue_qkv(layer + 1, 0)) if k else issue_down(layer, 6))
        gu_step(6, lambda k: more(lambda: issue_out(layer + 1, 0)) if k else more(lambda: issue_qkv(layer + 1, 1)), last=True)
        wait_slot(base + 18, 512, FF)
        scale2 = row_scale()
        for c0, w in tiles(FF, 512):
            gate = acc_g[:, c0:c0 + w] * scale2
            up = acc_u[:, c0:c0 + w] * scale2
            act[:, c0:c0 + w] = (gate * jax.nn.sigmoid(gate) * up).astype(BF16)

        def down_step(j, issue, lead):
            n = base + 18 + j
            s = slot_of(n)
            if lead:
                wait_slot(n, 512, FF)
            part = dot(act[:, :512], ring[s, :, :512])
            for b in range(1, 9):
                part = part + dot(act[:, b * 512:(b + 1) * 512], ring[s, :, b * 512:(b + 1) * 512])
            last = jnp.concatenate([ring[s, q * 128:(q + 1) * 128, 4608:4736] for q in range(4)], axis=1)
            part = part + dot(act[:, 4608:4736], last)
            stage_a(j, part)

            @pl.when(layer + 1 < LAYERS)
            def _():
                issue()

            if lead:
                stage_b(1, j - 1)

        down_step(0, lambda: issue_out(layer + 1, 1), False)

        def down_pair(t, carry):
            down_step(1 + 2 * t, lambda: issue_gu(layer + 1, t, 0), True)
            down_step(2 + 2 * t, lambda: issue_gu(layer + 1, t, 1), True)
            return carry

        lax.fori_loop(0, 3, down_pair, 0)
        stage_b(1, PAIRS - 1)
        return carry

    lax.fori_loop(0, LAYERS, layer_body, 0)

    stage_c(1, 0)

    def last_step(i, carry):
        @pl.when(i + 1 < PAIRS)
        def _():
            stage_c(1, i + 1)

        stage_d(i)
        for b in range(4):
            blk = 4 * i + b
            out[:, pl.ds(pl.multiple_of(blk * 128, 128), 128)] = x[blk]
        return carry

    lax.fori_loop(0, PAIRS, last_step, 0)


def fused_layers(x, positions, norm_attn, norm_mlp, wq, wk, wv, wo, wg, wu, wd, kc, vc):
    half = HD // 2
    freq = (np.float32(ROPE_BASE) ** (-np.arange(half, dtype=np.float32) / np.float32(half))).astype(np.float32)
    freq = jnp.asarray(np.concatenate([freq, freq])[None, :])
    hbm = pl.BlockSpec(memory_space=pl.ANY)
    vmem = pltpu.VMEM
    dma = pltpu.SemaphoreType.DMA
    scratch = [
        vmem((1, ROWS), jnp.int32), vmem((LAYERS, DIM), BF16), vmem((LAYERS, DIM), BF16), vmem((1, HD), F32), dma((4,)),
                vmem((SLOTS, 512, FF), BF16), dma((SLOTS,)),
        vmem((BLKS, ROWS, 128), BF16), dma,
        vmem((2 * LAYERS, PAIRS, 8, 128), F32),
        vmem((ROWS, HD), F32), vmem((ROWS, HD), F32), vmem((ROWS, HD), F32),
        vmem((ROWS, GROUP * CACHE), F32),
        vmem((ROWS, HD), F32),
        vmem((ROWS, HD), F32), vmem((ROWS, HD), F32), vmem((ROWS, QH * HD), BF16),
        vmem((ROWS, FF), F32), vmem((ROWS, FF), F32), vmem((ROWS, FF), BF16),
        dma((2,)),
        vmem((PAIRS, 2, ROWS, 128), BF16), vmem((PAIRS, 2, ROWS, 128), BF16),
        vmem((2, PAIRS, 2, ROWS, 128), BF16),
        dma((PAIRS,)), dma((PAIRS,)), dma((PAIRS,)), dma((2, PAIRS)), dma((PAIRS,)), dma((PAIRS,)),
    ]
    caches = vmem((LAYERS, ROWS * CACHE, HD), BF16)
    vm = pl.BlockSpec(memory_space=pltpu.VMEM)
    return pl.pallas_call(
        kernel,
        out_shape=(vmem((ROWS, DIM), BF16), caches, caches),
        in_specs=[hbm] * 14,
        out_specs=(vm, vm, vm),
        scratch_shapes=scratch,
        compiler_params=pltpu.CompilerParams(collective_id=0, has_side_effects=True, vmem_limit_bytes=59800000),
        name="layers",
    )(x, positions, norm_attn, norm_mlp, freq, wq, wk, wv, wo, wg, wu, wd, kc, vc)


def flush_kernel(x_ref, k_ref, v_ref, x_out, k_out, v_out, sem):
    pieces = [(x_ref, x_out)]
    for layer in range(LAYERS):
        pieces += [(k_ref.at[layer], k_out.at[layer]), (v_ref.at[layer], v_out.at[layer])]
    copies = [pltpu.make_async_copy(src, dst, sem.at[n]) for n, (src, dst) in enumerate(pieces)]
    for cp in copies:
        cp.start()
    for cp in copies:
        cp.wait()


def write_back(*arrays):
    return pl.pallas_call(
        flush_kernel,
        out_shape=tuple(jax.ShapeDtypeStruct(a.shape, a.dtype) for a in arrays),
        in_specs=[pl.BlockSpec(memory_space=pltpu.VMEM)] * 3,
        out_specs=(pl.BlockSpec(memory_space=pl.ANY),) * 3,
        scratch_shapes=[pltpu.SemaphoreType.DMA((1 + 2 * LAYERS,))],
        compiler_params=pltpu.CompilerParams(vmem_limit_bytes=16 * 2 ** 20),
        name="write_back",
    )(*arrays)


def solution(mesh):
    def local_step(hidden_in, positions, norm_attn, norm_mlp, w_query, w_key, w_value, w_out, w_gate, w_up, w_down, key_cache, value_cache):
        flat = (LAYERS, ROWS * CACHE, HD)
        hidden, k_out, v_out = fused_layers(
            hidden_in, positions[None, :], norm_attn, norm_mlp, w_query, w_key, w_value, w_out, w_gate, w_up, w_down,
            key_cache.reshape(flat), value_cache.reshape(flat))
        hidden, k_out, v_out = write_back(hidden, k_out, v_out)
        return hidden, k_out.reshape(key_cache.shape), v_out.reshape(value_cache.shape)

    row_spec = P("data", None)
    col_spec = P(None, None, "model")
    split_spec = P(None, "model", None)
    cache_spec = P(None, "data", None, "model", None)
    in_specs = (row_spec, P("data"), P(None, None), P(None, None), col_spec, col_spec, col_spec, split_spec, col_spec, col_spec, split_spec, cache_spec, cache_spec)
    out_specs = (row_spec, cache_spec, cache_spec)
    return jax.shard_map(local_step, mesh=mesh, in_specs=in_specs, out_specs=out_specs, check_vma=False)
```

```python
import functools

import jax
import jax.numpy as jnp
import numpy as np
from jax import lax
from jax.experimental import pallas as pl
from jax.experimental.pallas import tpu as pltpu
from jax.sharding import PartitionSpec as P

NORM_EPS = 1e-6
ROPE_BASE = 10000.0
MESH = pl.DeviceIdType.MESH
F32 = jnp.float32
BF16 = jnp.bfloat16

LAYERS = 3
ROWS = 128
DIM = 3584
HD = 128
QH = 7
CACHE = 32
FF = 4736
BLKS = DIM // 128
PAIRS = DIM // 512
QKV = (QH + 2) * HD
PER_LAYER = 2 + 2 + 2 * PAIRS + PAIRS
SLOTS = 10
DOWN = 2.0 ** -32
UP = 2.0 ** 32
GROUP = 8
GROUPS = ROWS // GROUP
QROWS = (QH + 1) * GROUP
KEYS = GROUP * CACHE


def kernel(x_hbm, pos_hbm, na_hbm, nm_hbm, freq_hbm, wq, wk, wv, wo, wg, wu, wd, kc_hbm, vc_hbm,
           out, kc_out, vc_out,
           pos_ref, na_ref, nm_ref, freq_ref, small_sem,
           ring, ring_sem, x, x_sem, gn, posb, cos_t, sin_t, vis, ss, kn, vn, ab, acc_g, acc_u, act,
           kv_sem, send, a_recv, b_recv, a_ss, a_rs, b_ss, b_rs, c_ss, c_rs):
    me = lax.axis_index("model")
    core = lax.rem(me, 2)
    partner = me + 1 - 2 * core
    peer = lax.rem(me + 2, 4)

    at = [acc_u.at[:, h * HD:(h + 1) * HD] for h in range(QH)]
    qs = [acc_u.at[:, (QH + h) * HD:(QH + h + 1) * HD] for h in range(QH)]
    qkv = acc_u.at[:, 2 * QH * HD:2 * QH * HD + QKV]
    sc = [acc_g.at[:QROWS, g * KEYS:(g + 1) * KEYS] for g in range(GROUPS)]
    pr = [act.at[:QROWS, g * KEYS:(g + 1) * KEYS] for g in range(GROUPS)]

    def slot_of(n):
        return lax.rem(n, SLOTS)

    def start(layer, r, src, rows, cols):
        s = slot_of(layer * PER_LAYER + r)
        pltpu.make_async_copy(src, ring.at[s, rows, cols], ring_sem.at[s]).start(priority=1)

    def issue_qkv(layer, r):
        for t in range(4 if r == 0 else 3):
            rows = slice((4 * r + t) * 512, (4 * r + t + 1) * 512)
            base = t * QKV
            start(layer, r, wq.at[layer, rows, :], slice(None), slice(base, base + QH * HD))
            start(layer, r, wk.at[layer, rows, :], slice(None), slice(base + QH * HD, base + (QH + 1) * HD))
            start(layer, r, wv.at[layer, rows, :], slice(None), slice(base + (QH + 1) * HD, base + QKV))

    def issue_out(layer, r):
        if r == 0:
            start(layer, 2, wo.at[layer, 0:512, :], slice(None), slice(0, DIM))
        else:
            start(layer, 3, wo.at[layer, 512:896, :], slice(0, 384), slice(0, DIM))

    def issue_gu(layer, i, which):
        rows = pl.ds(i * 512 if isinstance(i, int) else pl.multiple_of(i * 512, 512), 512)
        src = wu if which else wg
        start(layer, 4 + 2 * i + which, src.at[layer, rows, :], slice(None), slice(None))

    def issue_down(layer, j):
        off = j * 512 if isinstance(j, int) else pl.multiple_of(j * 512, 512)
        for b in range(9):
            start(layer, 18 + j, wd.at[layer, b * 512:(b + 1) * 512, pl.ds(off, 512)], slice(None), slice(b * 512, (b + 1) * 512))
        for q in range(4):
            cols = pl.ds(off + q * 128 if isinstance(j, int) else pl.multiple_of(off + q * 128, 128), 128)
            start(layer, 18 + j, wd.at[layer, 4608:4736, cols], slice(q * 128, (q + 1) * 128), slice(4608, 4736))

    def wait_slot(n, rows, cols):
        s = slot_of(n)
        pltpu.make_async_copy(wg.at[0, :rows, :cols], ring.at[s, :rows, :cols], ring_sem.at[s]).wait()

    def kv_copies(layer):
        return (pltpu.make_async_copy(kc_hbm.at[layer], kc_out.at[layer], kv_sem.at[0]),
                pltpu.make_async_copy(vc_hbm.at[layer], vc_out.at[layer], kv_sem.at[1]))

    barrier = pltpu.get_barrier_semaphore()
    for other in (partner, peer):
        pl.semaphore_signal(barrier, inc=1, device_id={"model": other}, device_id_type=MESH)

    small = [pltpu.make_async_copy(src, dst, small_sem.at[k]) for k, (src, dst) in enumerate((
        (pos_hbm, pos_ref), (na_hbm, na_ref), (nm_hbm, nm_ref), (freq_hbm, freq_ref)))]

    def load_x(b, carry):
        pltpu.make_async_copy(x_hbm.at[:, pl.ds(pl.multiple_of(b * 128, 128), 128)], x.at[b], x_sem).start()
        return carry


    issue_qkv(0, 0)
    for cp in small:
        cp.start()
    lax.fori_loop(0, BLKS, load_x, 0)
    issue_qkv(0, 1)
    for cp in kv_copies(0):
        cp.start()
    issue_out(0, 0)
    issue_out(0, 1)
    for k in range(6):
        issue_gu(0, k // 2, k % 2)

    for cp in small:
        cp.wait()
    for layer in range(LAYERS):
        for which, ref in enumerate((na_ref, nm_ref)):
            row = ref[layer:layer + 1, :].astype(F32) * DOWN
            for blk in range(BLKS):
                gn[2 * layer + which, blk // 4, blk % 4:blk % 4 + 1, :] = row[:, blk * 128:(blk + 1) * 128]
    pos_row = jnp.broadcast_to(pos_ref[...].astype(F32), (ROWS, ROWS))
    ri = lax.broadcasted_iota(jnp.int32, (ROWS, ROWS), 0)
    ci = lax.broadcasted_iota(jnp.int32, (ROWS, ROWS), 1)
    pos_col = jnp.sum(jnp.where(ri == ci, pos_row, 0.0), axis=1, keepdims=True)
    pos_b = jnp.broadcast_to(pos_col, (ROWS, HD))
    posb[...] = pos_b
    angle = pos_b * freq_ref[...]
    cos_t[...] = jnp.cos(angle)
    sin_v = jnp.sin(angle)
    sin_t[...] = jnp.where(ci < HD // 2, -sin_v, sin_v)
    r2 = lax.broadcasted_iota(jnp.int32, (ROWS, GROUP * CACHE), 0)
    c2 = lax.broadcasted_iota(jnp.int32, (ROWS, GROUP * CACHE), 1)
    mine = (c2 // CACHE) == lax.rem(r2, GROUP)
    seen = lax.rem(c2, CACHE).astype(F32) <= jnp.broadcast_to(pos_col, (ROWS, GROUP * CACHE))
    vis[...] = jnp.where(mine & seen, 1.0, 0.0)

    pltpu.make_async_copy(x, x, x_sem).wait()
    pl.semaphore_wait(barrier, 2)

    def a_copy(j):
        return pltpu.make_async_remote_copy(send.at[j], a_recv.at[j], a_ss.at[j], a_rs.at[j],
                                            device_id={"model": partner}, device_id_type=MESH)

    def b_copy(p, j):
        return pltpu.make_async_remote_copy(send.at[j], b_recv.at[p, j], b_ss.at[j], b_rs.at[p, j],
                                            device_id={"model": peer}, device_id_type=MESH)

    def c_copy(j, half):
        blk = pl.ds(4 * j + 2 * half, 2)
        return pltpu.make_async_remote_copy(x.at[blk], x.at[blk], c_ss.at[j], c_rs.at[j],
                                            device_id={"model": partner}, device_id_type=MESH)

    def own_cols(j, t):
        off = 2 * QH * HD + QKV + (2 * j + t) * 128
        return pl.ds(off if isinstance(j, int) else pl.multiple_of(off, 128), 128)

    def stage_a(j, part):
        first = core == 0
        for t in range(2):
            lo, hi = part[:, t * 128:(t + 1) * 128], part[:, (t + 2) * 128:(t + 3) * 128]
            acc_u[:, own_cols(j, t)] = jnp.where(first, lo, hi)
            send[j, t] = jnp.where(first, hi, lo).astype(BF16)
        a_copy(j).start()

    def stage_b(p, j):
        a_copy(j).wait_recv()
        a_copy(j).wait_send()
        for t in range(2):
            send[j, t] = (acc_u[:, own_cols(j, t)] + a_recv[j, t].astype(F32)).astype(BF16)
        b_copy(p, j).start()

    def stage_c(p, j):
        b_copy(p, j).wait_recv()
        total = send[j].astype(F32) + b_recv[p, j].astype(F32)
        blk = pl.ds(4 * j + 2 * core, 2)
        x[blk] = (x[blk].astype(F32) + total).astype(BF16)
        c_copy(j, core).start()
        b_copy(p, j).wait_send()

    def stage_d(j):
        c_copy(j, 1 - core).wait_recv()
        c_copy(j, core).wait_send()

    def take(row, i):
        outs = []
        sq = ss[...]
        gains = gn[row, i]
        for b in range(4):
            blk = x[4 * i + b].astype(F32)
            sq = sq + blk * blk
            outs.append((blk * gains[b:b + 1, :]).astype(BF16))
        ss[...] = sq
        return jnp.concatenate(outs, axis=1)

    def row_scale():
        mean = jnp.sum(ss[...], axis=1, keepdims=True) * (1.0 / DIM)
        return lax.rsqrt(mean + NORM_EPS) * UP

    def dot(a, b):
        return jnp.dot(a, b, preferred_element_type=F32)

    def tiles(width, step):
        return [(n, min(step, width - n)) for n in range(0, width, step)]

    def layer_body(layer, carry):
        base = layer * PER_LAYER
        ss[...] = jnp.zeros_like(ss)
        qkv[...] = jnp.zeros((ROWS, QKV), F32)

        @pl.when(layer > 0)
        def _():
            stage_c(1, 0)

        def qkv_step(i, carry):
            @pl.when((layer > 0) & (i + 1 < PAIRS))
            def _():
                stage_c(1, i + 1)

            @pl.when(layer > 0)
            def _():
                stage_d(i)

            h = take(2 * layer, i)
            s = slot_of(base + i // 4)
            first = lax.rem(i, 4) * QKV
            for c0, w in tiles(QKV, 512):
                qkv[:, c0:c0 + w] += dot(h, ring[s, :, pl.ds(pl.multiple_of(first + c0, 128), w)])
            return carry

        wait_slot(base, 512, 4 * QKV)
        lax.fori_loop(0, 4, qkv_step, 0)
        issue_gu(layer, 3, 0)
        wait_slot(base + 1, 512, 3 * QKV)
        lax.fori_loop(4, PAIRS, qkv_step, 0)
        issue_gu(layer, 3, 1)

        scale = row_scale()
        cos_v, sin_v = cos_t[...], sin_t[...]

        def head(idx):
            return (qkv[:, idx * HD:(idx + 1) * HD] * scale).astype(BF16)

        def rotate(v):
            v = v.astype(F32)
            return (v * cos_v + pltpu.roll(v, HD // 2, axis=1) * sin_v).astype(BF16)

        for h in range(QH):
            qs[h][...] = rotate(head(h)).astype(F32)
        k_new = rotate(head(QH))
        v_new = head(QH + 1)
        kn[...] = k_new.astype(F32)
        vn[...] = v_new.astype(F32)
        for cp in kv_copies(layer):
            cp.wait()
        wait_slot(base + 2, 512, DIM)
        wait_slot(base + 3, 384, DIM)
        srow = lax.broadcasted_iota(jnp.int32, (CACHE, HD), 0).astype(F32).astype(BF16)

        def spread(v):
            return jnp.broadcast_to(v[:, None, :], (GROUP, CACHE, HD)).reshape(GROUP * CACHE, HD)

        span = [slice(g * GROUP, (g + 1) * GROUP) for g in range(GROUPS)]
        cspan = [slice(g * KEYS, (g + 1) * KEYS) for g in range(GROUPS)]
        for t in range(ROWS):
            trow = slice(t * CACHE, (t + 1) * CACHE)
            here = srow == jnp.broadcast_to(posb[t:t + 1, :], (CACHE, HD)).astype(BF16)
            k_row = jnp.broadcast_to(kn[t:t + 1, :], (CACHE, HD)).astype(BF16)
            v_row = jnp.broadcast_to(vn[t:t + 1, :], (CACHE, HD)).astype(BF16)
            kc_out[layer, trow, :] = jnp.where(here, k_row, kc_out[layer, trow, :])
            vc_out[layer, trow, :] = jnp.where(here, v_row, vc_out[layer, trow, :])
        for g in range(GROUPS):
            q = jnp.concatenate([qs[h][span[g], :] for h in range(QH)] + [qs[0][span[g], :]], axis=0).astype(BF16)
            sc[g][...] = lax.dot_general(q, kc_out[layer, cspan[g], :], (((1,), (1,)), ((), ())), preferred_element_type=F32)
        for g in range(GROUPS):
            raw = (sc[g][...] * (HD ** -0.5)).reshape(QH + 1, GROUP, KEYS)
            raw = jnp.where((vis[span[g], :] > 0.5)[None], raw, -1e30)
            e = jnp.exp(raw - jnp.max(raw, axis=-1, keepdims=True))
            prob = e * (1.0 / jnp.sum(e, axis=-1, keepdims=True))
            pr[g][...] = prob.reshape(QROWS, KEYS).astype(BF16)
        for g in range(GROUPS):
            o = dot(pr[g][...], vc_out[layer, cspan[g], :])
            for h in range(QH):
                at[h][span[g], :] = o[h * GROUP:(h + 1) * GROUP]

        for h in range(QH):
            ab[:, h * HD:(h + 1) * HD] = at[h][...].astype(BF16)

        for j in range(PAIRS):
            cols = slice(j * 512, (j + 1) * 512)
            part = dot(ab[:, :512], ring[slot_of(base + 2), :, cols]) + dot(ab[:, 512:], ring[slot_of(base + 3), :384, cols])
            stage_a(j, part)
            if j >= 2:
                stage_b(0, j - 2)
        issue_gu(layer, 4, 0)
        issue_gu(layer, 4, 1)
        for j in range(PAIRS - 2, PAIRS):
            stage_b(0, j)

        ss[...] = jnp.zeros_like(ss)
        stage_c(0, 0)

        def gu_step(i, issue, first=False, last=False):
            if not last:
                stage_c(0, i + 1)
            stage_d(i)
            h = take(2 * layer + 1, i)
            n = base + 4 + 2 * i
            wait_slot(n, 512, FF)
            wait_slot(n + 1, 512, FF)
            for k, acc in ((0, acc_g), (1, acc_u)):
                s = slot_of(n + k)
                for c0, w in tiles(FF, 512):
                    part = dot(h, ring[s, :, c0:c0 + w])
                    if first:
                        acc[:, c0:c0 + w] = part
                    else:
                        acc[:, c0:c0 + w] += part
            issue(0)
            issue(1)

        gu_step(0, lambda k: issue_gu(layer, 5, k), first=True)
        gu_step(1, lambda k: issue_gu(layer, 6, k))

        def gu_mid(i, carry):
            gu_step(i, lambda k: issue_down(layer, 2 * (i - 2) + k))
            return carry

        lax.fori_loop(2, 5, gu_mid, 0)

        def more(fn):
            pl.when(layer + 1 < LAYERS)(fn)

        gu_step(5, lambda k: more(lambda: issue_qkv(layer + 1, 0)) if k else issue_down(layer, 6))
        gu_step(6, lambda k: more(lambda: issue_out(layer + 1, 0)) if k else more(lambda: issue_qkv(layer + 1, 1)), last=True)
        wait_slot(base + 18, 512, FF)
        @pl.when(layer + 1 < LAYERS)
        def _():
            for cp in kv_copies(layer + 1):
                cp.start()

        scale2 = row_scale()
        for c0, w in tiles(FF, 512):
            gate = acc_g[:, c0:c0 + w] * scale2
            up = acc_u[:, c0:c0 + w] * scale2
            act[:, c0:c0 + w] = (gate * jax.nn.sigmoid(gate) * up).astype(BF16)

        def down_step(j, issue, lead):
            n = base + 18 + j
            s = slot_of(n)
            if lead:
                wait_slot(n, 512, FF)
            part = dot(act[:, :512], ring[s, :, :512])
            for b in range(1, 9):
                part = part + dot(act[:, b * 512:(b + 1) * 512], ring[s, :, b * 512:(b + 1) * 512])
            last = jnp.concatenate([ring[s, q * 128:(q + 1) * 128, 4608:4736] for q in range(4)], axis=1)
            part = part + dot(act[:, 4608:4736], last)
            stage_a(j, part)

            @pl.when(layer + 1 < LAYERS)
            def _():
                issue()

            if lead:
                stage_b(1, j - 1)

        down_step(0, lambda: issue_out(layer + 1, 1), False)

        def down_pair(t, carry):
            down_step(1 + 2 * t, lambda: issue_gu(layer + 1, t, 0), True)
            down_step(2 + 2 * t, lambda: issue_gu(layer + 1, t, 1), True)
            return carry

        lax.fori_loop(0, 3, down_pair, 0)
        stage_b(1, PAIRS - 1)
        return carry

    lax.fori_loop(0, LAYERS, layer_body, 0)

    stage_c(1, 0)

    def last_step(i, carry):
        @pl.when(i + 1 < PAIRS)
        def _():
            stage_c(1, i + 1)

        stage_d(i)
        for b in range(4):
            blk = 4 * i + b
            out[:, pl.ds(pl.multiple_of(blk * 128, 128), 128)] = x[blk]
        return carry

    lax.fori_loop(0, PAIRS, last_step, 0)


def fused_layers(x, positions, norm_attn, norm_mlp, wq, wk, wv, wo, wg, wu, wd, kc, vc):
    half = HD // 2
    freq = (np.float32(ROPE_BASE) ** (-np.arange(half, dtype=np.float32) / np.float32(half))).astype(np.float32)
    freq = jnp.asarray(np.concatenate([freq, freq])[None, :])
    hbm = pl.BlockSpec(memory_space=pl.ANY)
    vmem = pltpu.VMEM
    dma = pltpu.SemaphoreType.DMA
    scratch = [
        vmem((1, ROWS), jnp.int32), vmem((LAYERS, DIM), BF16), vmem((LAYERS, DIM), BF16), vmem((1, HD), F32), dma((4,)),
                vmem((SLOTS, 512, FF), BF16), dma((SLOTS,)),
        vmem((BLKS, ROWS, 128), BF16), dma,
        vmem((2 * LAYERS, PAIRS, 8, 128), F32),
        vmem((ROWS, HD), F32), vmem((ROWS, HD), F32), vmem((ROWS, HD), F32),
        vmem((ROWS, GROUP * CACHE), F32),
        vmem((ROWS, HD), F32),
        vmem((ROWS, HD), F32), vmem((ROWS, HD), F32), vmem((ROWS, QH * HD), BF16),
        vmem((ROWS, FF), F32), vmem((ROWS, FF), F32), vmem((ROWS, FF), BF16),
        dma((2,)),
        vmem((PAIRS, 2, ROWS, 128), BF16), vmem((PAIRS, 2, ROWS, 128), BF16),
        vmem((2, PAIRS, 2, ROWS, 128), BF16),
        dma((PAIRS,)), dma((PAIRS,)), dma((PAIRS,)), dma((2, PAIRS)), dma((PAIRS,)), dma((PAIRS,)),
    ]
    caches = vmem((LAYERS, ROWS * CACHE, HD), BF16)
    vm = pl.BlockSpec(memory_space=pltpu.VMEM)
    return pl.pallas_call(
        kernel,
        out_shape=(vmem((ROWS, DIM), BF16), caches, caches),
        in_specs=[hbm] * 14,
        out_specs=(vm, vm, vm),
        scratch_shapes=scratch,
        compiler_params=pltpu.CompilerParams(collective_id=0, has_side_effects=True, vmem_limit_bytes=59800000),
        name="layers",
    )(x, positions, norm_attn, norm_mlp, freq, wq, wk, wv, wo, wg, wu, wd, kc, vc)


def flush_kernel(x_ref, k_ref, v_ref, x_out, k_out, v_out, sem):
    pieces = [(x_ref, x_out)]
    for layer in range(LAYERS):
        pieces += [(k_ref.at[layer], k_out.at[layer]), (v_ref.at[layer], v_out.at[layer])]
    copies = [pltpu.make_async_copy(src, dst, sem.at[n]) for n, (src, dst) in enumerate(pieces)]
    for cp in copies:
        cp.start()
    for cp in copies:
        cp.wait()


def write_back(*arrays):
    return pl.pallas_call(
        flush_kernel,
        out_shape=tuple(jax.ShapeDtypeStruct(a.shape, a.dtype) for a in arrays),
        in_specs=[pl.BlockSpec(memory_space=pltpu.VMEM)] * 3,
        out_specs=(pl.BlockSpec(memory_space=pl.ANY),) * 3,
        scratch_shapes=[pltpu.SemaphoreType.DMA((1 + 2 * LAYERS,))],
        compiler_params=pltpu.CompilerParams(vmem_limit_bytes=16 * 2 ** 20),
        name="write_back",
    )(*arrays)


def solution(mesh):
    def local_step(hidden_in, positions, norm_attn, norm_mlp, w_query, w_key, w_value, w_out, w_gate, w_up, w_down, key_cache, value_cache):
        flat = (LAYERS, ROWS * CACHE, HD)
        hidden, k_out, v_out = fused_layers(
            hidden_in, positions[None, :], norm_attn, norm_mlp, w_query, w_key, w_value, w_out, w_gate, w_up, w_down,
            key_cache.reshape(flat), value_cache.reshape(flat))
        hidden, k_out, v_out = write_back(hidden, k_out, v_out)
        return hidden, k_out.reshape(key_cache.shape), v_out.reshape(value_cache.shape)

    row_spec = P("data", None)
    col_spec = P(None, None, "model")
    split_spec = P(None, "model", None)
    cache_spec = P(None, "data", None, "model", None)
    in_specs = (row_spec, P("data"), P(None, None), P(None, None), col_spec, col_spec, col_spec, split_spec, col_spec, col_spec, split_spec, cache_spec, cache_spec)
    out_specs = (row_spec, cache_spec, cache_spec)
    return jax.shard_map(local_step, mesh=mesh, in_specs=in_specs, out_specs=out_specs, check_vma=False)
```
